32 devices in a mesh: grp: 4 (over y, x), dev: 8 (over z, core).
Axes of the slice: x: 2, y: 2, z: 4, core: 2. Of those that a mesh axis runs over, the one named last changes fastest.
Arguments:
- load: float32 [1024, 256, 128], P('grp', 'dev'), may hold values from -11 to 11
- east_class: int32 [1024, 256], P('grp', 'dev'), may hold values from 0 to 7
- north_class: int32 [1024, 256], P('grp', 'dev'), may hold values from 0 to 7
- cond_table: float32 [8], replicated, may hold values from 0.25 to 4
- taps: int32 [128, 16], replicated, may hold values from 0 to 262143
- tap_current: float32 [128, 16], replicated, may hold values from -16 to 16
Outputs:
- potential: float32 [1024, 256, 128], P('grp', 'dev')
The draws below stay inside these ranges and needn't reach their ends.
Inputs may be any that keep to these rules, and one draw needn't show every extreme that they name: `taps`: tap number i * 256 + j stands for node (i, j).
All inputs are finite; a program needn't handle non-finite values.
Results may differ from the reference program's by a relative error of at most 0.0001.
Values sent between devices are 32-bit elements; how exact they have to be, the bound alone decides.
No kernel may reach another device: no remote copies, remote signals or barrier semaphores. Data moves between devices by JAX's collectives and lax.ppermute only.
A program may use at most 128 MiB of HBM per device.

```python
import math
import jax
import jax.numpy as jnp
from jax import lax

C = 128
CLASSES = 8
TAPS = 16
LEVELS = 5
NX = 1024
NY = 256


def draw_load(key, part):
    first_key = jax.random.fold_in(jax.random.fold_in(key, 17), 0)
    rough = 1.5 * jnp.clip(jax.random.normal(first_key, (NX, NY, C), jnp.float32), -4.0, 4.0)
    return rough


def with_ends(entries, stream_key, low, high):
    index_at = [jax.random.randint(jax.random.fold_in(stream_key, axis), (), 0, length) for axis, length in enumerate(entries.shape)]
    main_axis = entries.shape.index(max(entries.shape))
    beside = index_at[:main_axis] + [(index_at[main_axis] + 1) % entries.shape[main_axis]] + index_at[main_axis + 1:]
    return entries.at[tuple(index_at)].set(low).at[tuple(beside)].set(high)


def bell_draw(rng, extent, scale, reach, kind=jnp.bfloat16):
    drawn = scale * jax.random.normal(rng, extent, jnp.float32)
    return jnp.clip(drawn, min=-reach, max=reach).astype(kind)


def setup_inputs(seed: int = 0) -> dict:
    arg_keys = jax.random.split(jax.random.key(seed), 7)
    return {
        "load": draw_load(jax.random.fold_in(arg_keys[6], 71), 0),
        "east_class": with_ends(jax.random.randint(arg_keys[1], (NX, NY), 0, CLASSES), jax.random.fold_in(arg_keys[1], 1), 0, CLASSES - 1).astype(jnp.int32),
        "north_class": with_ends(jax.random.randint(arg_keys[2], (NX, NY), 0, CLASSES), jax.random.fold_in(arg_keys[2], 1), 0, CLASSES - 1).astype(jnp.int32),
        "cond_table": jnp.clip(jnp.exp(jax.random.uniform(arg_keys[3], (CLASSES,), jnp.float32, math.log(0.25), math.log(4.0))), 0.25, 4.0),
        "taps": with_ends(jax.random.randint(arg_keys[4], (C, TAPS), 0, NX * NY), jax.random.fold_in(arg_keys[4], 1), 0, (NX * NY) - 1).astype(jnp.int32),
        "tap_current": bell_draw(arg_keys[5], (C, TAPS), 4.0, 16.0, jnp.float32),
    }


RELAXATION = 0.8
SHUNT_CONDUCT = 0.01

def diagonal_of(east_cond, north_cond, shunt):
    west_cond = jnp.pad(east_cond, ((1, 0), (0, 0)))[:-1]
    south_cond = jnp.pad(north_cond, ((0, 0), (1, 0)))[:, :-1]
    return shunt + east_cond + west_cond + north_cond + south_cond

def operate(potential, east_cond, north_cond, shunt):
    padded = jnp.pad(potential, ((1, 1), (1, 1), (0, 0)))
    west_cond = jnp.pad(east_cond, ((1, 0), (0, 0)))[:-1]
    south_cond = jnp.pad(north_cond, ((0, 0), (1, 0)))[:, :-1]
    diagonal = shunt + east_cond + west_cond + north_cond + south_cond
    applied = diagonal[..., None] * potential - east_cond[..., None] * padded[2:, 1:-1] - west_cond[..., None] * padded[:-2, 1:-1] - north_cond[..., None] * padded[1:-1, 2:] - south_cond[..., None] * padded[1:-1, :-2]
    return (applied, diagonal)

def relax(potential, source, east_cond, north_cond, shunt):
    applied, diagonal = operate(potential, east_cond, north_cond, shunt)
    return potential + RELAXATION * (source - applied) / diagonal[..., None]

def restrict(values):
    row_count, col_count, cand_count = values.shape
    return values.reshape(row_count // 2, 2, col_count // 2, 2, cand_count).sum(axis=(1, 3))

def prolong(values):
    return jnp.repeat(jnp.repeat(values, 2, axis=0), 2, axis=1)

def coarsen(east_cond, north_cond):
    row_count, col_count = east_cond.shape
    coarse_east = east_cond.reshape(row_count // 2, 2, col_count // 2, 2)[:, 1].sum(axis=-1)
    coarse_north = north_cond.reshape(row_count // 2, 2, col_count // 2, 2)[:, :, :, 1].sum(axis=1)
    return (coarse_east, coarse_north)

def coarse_factor(east_cond, north_cond, shunt):
    row_count, col_count = east_cond.shape
    node_count = row_count * col_count
    diagonal = diagonal_of(east_cond, north_cond, shunt).reshape(-1)
    east_flat = east_cond.reshape(-1)
    north_flat = north_cond.reshape(-1)
    matrix = jnp.diag(diagonal) - jnp.diag(east_flat[:node_count - col_count], col_count) - jnp.diag(east_flat[:node_count - col_count], -col_count) - jnp.diag(north_flat[:node_count - 1], 1) - jnp.diag(north_flat[:node_count - 1], -1)
    return jnp.linalg.cholesky(matrix)

def vcycle(source, conduct_list, factor):
    stored = []
    for height in range(LEVELS):
        east_cond, north_cond = conduct_list[height]
        shunt = SHUNT_CONDUCT * 4.0 ** height
        diagonal = diagonal_of(east_cond, north_cond, shunt)
        initial = RELAXATION * source / diagonal[..., None]
        potential = relax(initial, source, east_cond, north_cond, shunt)
        applied = operate(potential, east_cond, north_cond, shunt)[0]
        stored.append((potential, source))
        source = restrict(source - applied)
    row_count, col_count = conduct_list[LEVELS][0].shape
    correction = jax.scipy.linalg.cho_solve((factor, True), source.reshape(row_count * col_count, -1))
    correction = correction.reshape(row_count, col_count, -1)
    for height in reversed(range(LEVELS)):
        east_cond, north_cond = conduct_list[height]
        shunt = SHUNT_CONDUCT * 4.0 ** height
        potential, source = stored[height]
        potential = potential + prolong(correction)
        for iteration in range(2):
            potential = relax(potential, source, east_cond, north_cond, shunt)
        correction = potential
    return correction

def reference(load, east_class, north_class, cond_table, taps, tap_current):
    east_cond = cond_table[east_class].at[-1, :].set(0.0)
    north_cond = cond_table[north_class].at[:, -1].set(0.0)
    conduct_list = [(east_cond, north_cond)]
    for height in range(LEVELS):
        conduct_list.append(coarsen(*conduct_list[-1]))
    factor = coarse_factor(*conduct_list[LEVELS], SHUNT_CONDUCT * 4.0 ** LEVELS)
    per_block = 16

    def solve_block(block_index):
        offset = block_index * per_block
        block_load = lax.dynamic_slice_in_dim(load, offset, per_block, 2)
        block_taps = lax.dynamic_slice_in_dim(taps, offset, per_block, 0)
        block_amps = lax.dynamic_slice_in_dim(tap_current, offset, per_block, 0)
        columns = jnp.broadcast_to(jnp.arange(per_block, dtype=jnp.int32)[:, None], block_taps.shape)
        injected = jnp.zeros((NX * NY, per_block), load.dtype).at[block_taps, columns].add(block_amps)
        source = injected.reshape(NX, NY, per_block) - block_load
        return vcycle(source, conduct_list, factor)
    solved = lax.map(solve_block, jnp.arange(C // per_block, dtype=jnp.int32))
    return jnp.moveaxis(solved, 0, 2).reshape(NX, NY, C)
```

```python
import functools

import jax
import jax.numpy as jnp
from jax import lax
from jax.experimental import pallas as pl
from jax.experimental.pallas import tpu as pltpu
from jax.sharding import PartitionSpec as P

LEVELS = 5
RELAXATION = 0.8
KEEP = 1.0 - RELAXATION
SHUNT_CONDUCT = 0.01
AXES = ("grp", "dev")
HIGH = lax.Precision.HIGHEST

HALO = 10
PAD = 16
LANES = 128
GROUP = 8


def exchange(tail, head, axis):
    count = lax.axis_size(axis)
    up = [(i, i + 1) for i in range(count - 1)]
    down = [(i + 1, i) for i in range(count - 1)]
    return lax.ppermute(tail, axis, up), lax.ppermute(head, axis, down)


def pack(rows, extra):
    flat = extra.reshape(-1)
    size = -flat.shape[0] % LANES
    return jnp.concatenate([rows.reshape(-1, LANES), jnp.pad(flat, (0, size)).reshape(-1, LANES)])


def unpack(packed, rows, extra):
    count = rows.size // LANES
    flat = packed[count:].reshape(-1)[: extra.size]
    return packed[:count].reshape(rows.shape), flat.reshape(extra.shape)


def pair_matrix(count, half, first=0, odd_only=False):
    fine = jnp.arange(count)[:, None] - first
    coarse = jnp.arange(half)[None, :]
    hit = fine == 2 * coarse + 1 if odd_only else fine // 2 == coarse
    return hit.astype(jnp.float32)


def stencil_coefs(east, north, shunt):
    west = east[:, :-1]
    east = east[:, 1:]
    north = north[:, 1:]
    south = jnp.pad(north, ((1, 0), (0, 0)))[:-1]
    diag = shunt + east + west + north + south
    coefs = jnp.stack([east, west, north, south, RELAXATION / diag, diag])
    rows = coefs.shape[2]
    tiles = -(-rows // LANES)
    coefs = jnp.pad(coefs, ((0, 0), (0, 0), (0, tiles * LANES - rows)))
    return jnp.moveaxis(coefs.reshape(6, coefs.shape[1], tiles, LANES), 2, 1)


def row_coefs(ref, kinds, g):
    per_tile = LANES // GROUP
    shift = lax.rem(LANES - lax.rem(g, per_tile) * GROUP, LANES)
    return [pltpu.roll(ref[k, g // per_tile], shift, 1) for k in kinds]


def spread(coef, r):
    return jnp.broadcast_to(coef[:, r : r + 1], coef.shape)


def around(ref, row, cols, coefs):
    east, west, north, south = coefs
    here = ref[row, cols, :]
    count = here.shape[0]
    total = east * ref[row + 1, cols, :] + west * ref[row - 1, cols, :]
    total += north * pltpu.roll(here, count - 1, 0) + south * pltpu.roll(here, 1, 0)
    return here, total


def down_kernel(
    dims, tap_count, tap_code, tap_amps, own, west, east, north, south, corners, coef0, coef1,
    s0, p0, s1, p1, slab, u0, u1, s2, pair, pair1,
):
    rows, cols, nd, pc = dims
    wide = cols + 2 * PAD
    everything = slice(None)

    zero_side = jnp.zeros((s0.shape[0], PAD, LANES), jnp.float32)
    s0[:, 0:PAD, :] = zero_side
    s0[:, PAD + cols :, :] = zero_side
    tail = s0.shape[0] - (rows + 2 * HALO)
    s0[rows + 2 * HALO :, :, :] = jnp.zeros((tail, wide, LANES), jnp.float32)
    s0[HALO : HALO + rows, PAD : PAD + cols, :] = -own[...]
    s0[0:HALO, PAD : PAD + cols, :] = -north[...]
    s0[HALO + rows : rows + 2 * HALO, PAD : PAD + cols, :] = -south[...]
    flat = s0.reshape(s0.shape[0] * wide, LANES)
    for j in range(HALO):
        for side, (strip, first) in enumerate(((west, PAD - HALO), (east, PAD + cols))):
            flat[pl.ds(HALO * wide + first + j, rows, stride=wide), :] = -strip[j]
            for end, base in enumerate((0, HALO + rows)):
                block = corners[side, end, j * HALO : (j + 1) * HALO, :]
                flat[pl.ds(base * wide + first + j, HALO, stride=wide), :] = -block

    lane = lax.broadcasted_iota(jnp.int32, (GROUP, LANES), 1)
    sub = lax.broadcasted_iota(jnp.int32, (GROUP, LANES), 0)

    def add_tap(k, carry):
        code = tap_code[k]
        node = code // LANES
        base = pl.multiple_of(node // GROUP * GROUP, GROUP)
        hit = (lane == lax.rem(code, LANES)) & (sub == node - base)
        flat[pl.ds(base, GROUP), :] += jnp.where(hit, tap_amps[k], 0.0)
        return carry

    lax.fori_loop(0, tap_count[0], add_tap, 0)

    def smooth_and_restrict(source, start, pre, coef, pair, store):
        width = source.shape[1]
        groups = source.shape[0] // GROUP
        zero = jnp.zeros((width, LANES), jnp.float32)
        last = pre.shape[0] - 1
        for ref in (start, pre):
            ref[0] = zero
            ref[last] = zero

        def first(g, carry):
            (weight,) = row_coefs(coef, (4,), g)
            for r in range(GROUP):
                row = g * GROUP + r
                start[row + 1] = spread(weight, r) * source[row]
            return carry

        def second(g, carry):
            found = row_coefs(coef, (0, 1, 2, 3, 4), g)
            for r in range(GROUP):
                row = g * GROUP + r
                c = [spread(x, r) for x in found]
                _, total = around(start, row + 1, everything, c[:4])
                pre[row + 1] = c[4] * ((2.0 - RELAXATION) * source[row] + total)
            return carry

        def third(g, carry):
            found = row_coefs(coef, (0, 1, 2, 3, 5), g)
            for m in range(GROUP // 2):
                both = None
                for r in (2 * m, 2 * m + 1):
                    row = g * GROUP + r
                    c = [spread(x, r) for x in found]
                    here, total = around(pre, row + 1, everything, c[:4])
                    rest = source[row] - c[4] * here + total
                    both = rest if both is None else both + rest
                pair[m] = both
                store(g * (GROUP // 2) + m, m)
            return carry

        lax.fori_loop(0, groups, first, 0)
        lax.fori_loop(0, groups, second, 0)
        lax.fori_loop(0, groups, third, 0)

    half = (cols + 2 * (HALO - 2)) // 2
    s1[...] = jnp.zeros_like(s1)

    def store1(k, m):
        first = PAD - (HALO - 2)
        s1[k + 1] = pair[m, pl.ds(first, half, stride=2), :] + pair[m, pl.ds(first + 1, half, stride=2), :]

    smooth_and_restrict(s0, u0, p0, coef0, pair, store1)
    quarter = cols // 4

    def store2(k, m):
        s2[pl.ds(pl.multiple_of(k * quarter, quarter), quarter), :] = (
            pair1[m, pl.ds(4, quarter, stride=2), :] + pair1[m, pl.ds(5, quarter, stride=2), :]
        )

    smooth_and_restrict(s1, u1, p1, coef1, pair1, store2)
    rows2 = rows // 4
    per = LANES // rows2
    groups = quarter // per
    for jp in range(groups):
        parts = [
            s2[pl.ds(3 * quarter + jl * groups + jp, rows2, stride=quarter), :] for jl in range(per)
        ]
        turned = jnp.concatenate(parts, axis=0).T
        for p in range(pc):
            slab[pl.ds(jp * pc + p, nd, stride=groups * pc), :] = turned[p * nd : (p + 1) * nd]


def up_kernel(dims, back, s0, p0, s1, p1, coef0, coef1, out, x2, v1a, v1b, wide1, v0a, v0b):
    rows, cols, nd, pc = dims
    quarter = cols // 4
    wide2 = quarter + 4
    pitch2 = x2.shape[0] // (rows // 4 + 4)
    for jw in range(wide2):
        parts = [back[pl.ds(jw * pc + p, nd, stride=wide2 * pc), :] for p in range(pc)]
        turned = jnp.concatenate(parts, axis=0).T
        x2[pl.ds(jw, rows // 4 + 4, stride=pitch2), :] = turned[: rows // 4 + 4]

    def step(source, old, new, coef, cols_at, source_cols, lo, hi):
        def go(g, carry):
            found = row_coefs(coef, (0, 1, 2, 3, 4), g)
            found = [f[cols_at] for f in found]
            for r in range(GROUP):
                row = g * GROUP + r
                c = [spread(x, r) for x in found]
                here, total = around(old, row + 1, slice(None), c[:4])
                new[row + 1] = KEEP * here + c[4] * (source[row, source_cols, :] + total)
            return carry

        lax.fori_loop(lo, hi, go, 0)

    v1a[...] = jnp.zeros_like(v1a)
    v1b[...] = jnp.zeros_like(v1b)
    width1 = 2 * wide2

    def lift1(k, carry):
        x = x2[pl.ds(k * pitch2, pitch2), :][:wide2]
        wide1[pl.ds(0, wide2, stride=2), :] = x
        wide1[pl.ds(1, wide2, stride=2), :] = x
        both = wide1[0:width1, :]
        for r in range(2):
            row = 2 * k + 3 + r
            v1a[row] = p1[row] + both
        return carry

    lax.fori_loop(0, rows // 4 + 4, lift1, 0)
    whole = slice(None)
    step(s1, v1a, v1b, coef1, whole, whole, 0, s1.shape[0] // GROUP)
    step(s1, v1b, v1a, coef1, whole, whole, 0, s1.shape[0] // GROUP)

    width0 = 2 * width1
    left = PAD - (HALO - 2)
    window = slice(left, left + width0)
    first = HALO // GROUP
    last = -(-(HALO + rows + 1) // GROUP)

    def lift0(k, carry):
        x = v1a[k + 6]
        wide1[pl.ds(0, width1, stride=2), :] = x
        wide1[pl.ds(1, width1, stride=2), :] = x
        both = wide1[...]
        for r in range(2):
            row = 2 * k + HALO - 2 + r + 1
            v0a[row] = p0[row, window, :] + both
        return carry

    v0a[first * GROUP] = jnp.zeros((width0, LANES), jnp.float32)
    for row in range(rows + HALO + 2 + 1, v0a.shape[0]):
        v0a[row] = jnp.zeros((width0, LANES), jnp.float32)
    lax.fori_loop(0, rows // 2 + 2, lift0, 0)
    v0b[first * GROUP] = jnp.zeros((width0, LANES), jnp.float32)
    step(s0, v0a, v0b, coef0, window, window, first, last)
    v0b[last * GROUP + 1] = jnp.zeros((width0, LANES), jnp.float32)

    own = slice(PAD - left, PAD - left + cols)

    def finish(g, carry):
        found = [f[window] for f in row_coefs(coef0, (0, 1, 2, 3, 4), g)]
        for r in range(GROUP):
            row = g * GROUP + r
            c = [spread(x, r) for x in found]
            here, total = around(v0b, row + 1, slice(None), c[:4])
            done = KEEP * here + c[4] * (s0[row, window, :] + total)

            @pl.when((row >= HALO) & (row < HALO + rows))
            def _():
                out[row - HALO] = done[own]

        return carry

    lax.fori_loop(first, last, finish, 0)


VMEM = pl.BlockSpec(memory_space=pltpu.VMEM)
SMEM = pl.BlockSpec(memory_space=pltpu.SMEM)
PARAMS = pltpu.CompilerParams(vmem_limit_bytes=60 * 2**20)


def shape(*dims):
    return jax.ShapeDtypeStruct(dims, jnp.float32)


def vmem(*dims):
    return pltpu.VMEM(dims, jnp.float32)


def operate_lead(v, east, north, shunt):
    padded = jnp.pad(v, ((0, 0), (1, 1), (1, 1)))
    west = jnp.pad(east, ((0, 0), (1, 0)))[:, :-1]
    south = jnp.pad(north, ((1, 0), (0, 0)))[:-1]
    diag = shunt + east + west + north + south
    applied = (
        diag * v
        - east * padded[:, 1:-1, 2:]
        - west * padded[:, 1:-1, :-2]
        - north * padded[:, 2:, 1:-1]
        - south * padded[:, :-2, 1:-1]
    )
    return applied, diag


def relax_lead(v, source, east, north, shunt):
    applied, diag = operate_lead(v, east, north, shunt)
    return v + RELAXATION * (source - applied) / diag


def coarse_cycle(source, east, north, level):
    shunt = SHUNT_CONDUCT * 4.0**level
    count, nj, ni = source.shape
    if level == LEVELS:
        size = nj * ni
        west = jnp.pad(east, ((0, 0), (1, 0)))[:, :-1]
        south = jnp.pad(north, ((1, 0), (0, 0)))[:-1]
        diag = (shunt + east + west + north + south).reshape(-1)
        e = east.reshape(-1)[: size - 1]
        n = north.reshape(-1)[: size - ni]
        matrix = (
            jnp.diag(diag) - jnp.diag(e, 1) - jnp.diag(e, -1) - jnp.diag(n, ni) - jnp.diag(n, -ni)
        )
        factor = jnp.linalg.cholesky(matrix)
        solved = jax.scipy.linalg.cho_solve((factor, True), source.reshape(count, size).T)
        return solved.T.reshape(source.shape)
    _, diag = operate_lead(source, east, north, shunt)
    pre = relax_lead(RELAXATION * source / diag, source, east, north, shunt)
    rest = source - operate_lead(pre, east, north, shunt)[0]
    pi = pair_matrix(ni, ni // 2)
    pj = pair_matrix(nj, nj // 2)
    dot = functools.partial(jnp.einsum, precision=HIGH)
    coarse = dot("pji,jJ,iI->pJI", rest, pj, pi)
    east1 = dot("ji,jJ,iI->JI", east, pj, pair_matrix(ni, ni // 2, odd_only=True))
    north1 = dot("ji,jJ,iI->JI", north, pair_matrix(nj, nj // 2, odd_only=True), pi)
    fix = coarse_cycle(coarse, east1, north1, level + 1)
    v = pre + dot("pJI,jJ,iI->pji", fix, pj, pi)
    v = relax_lead(v, source, east, north, shunt)
    return relax_lead(v, source, east, north, shunt)


def live_taps(taps, tap_current, rows, cols, row_start, col_start, all_cols):
    i = taps // all_cols - row_start
    j = taps % all_cols - col_start
    inside = (i >= -HALO) & (i < rows + HALO) & (j >= -HALO) & (j < cols + HALO)
    cand = lax.broadcasted_iota(jnp.int32, taps.shape, 0)
    code = ((i + HALO) * (cols + 2 * PAD) + j + PAD) * LANES + cand
    count = taps.size
    lead = count // LANES
    flags = inside.reshape(lead, LANES).astype(jnp.float32)
    upto = jnp.dot(flags, jnp.triu(jnp.ones((LANES, LANES), jnp.float32)), precision=HIGH)
    before = jnp.dot(
        jnp.tril(jnp.ones((lead, lead), jnp.float32), -1), upto[:, -1:], precision=HIGH
    )
    place = (upto + before).astype(jnp.int32).reshape(-1)
    place = jnp.where(inside.reshape(-1), place - 1, -1)
    pick = place[None, :] == jnp.arange(count, dtype=jnp.int32)[:, None]
    codes = jnp.sum(jnp.where(pick, code.reshape(-1)[None], 0), axis=1)
    amps = jnp.sum(jnp.where(pick, tap_current.reshape(-1)[None], 0.0), axis=1)
    return jnp.sum(inside.astype(jnp.int32)).reshape(1), codes, amps


def body(load, east_class, north_class, cond_table, taps, tap_current):
    rows, cols, cands = load.shape
    ng, nd_axis = lax.axis_size("grp"), lax.axis_size("dev")
    nd = ng * nd_axis
    pc = cands // nd
    row_start = lax.axis_index("grp") * rows
    col_start = lax.axis_index("dev") * cols
    all_rows, all_cols = ng * rows, nd_axis * cols
    edge = HALO + 1
    dims = (rows, cols, nd, pc)

    classes = jnp.stack([east_class.T, north_class.T]).astype(jnp.float32)
    strip_w = jnp.swapaxes(load[:, :HALO], 0, 1)
    strip_e = jnp.swapaxes(load[:, cols - HALO :], 0, 1)
    from_w, from_e = exchange(
        pack(strip_e, classes[:, cols - edge :]), pack(strip_w, classes[:, :edge]), "dev"
    )
    from_n, from_s = exchange(
        pack(load[rows - HALO :], classes[:, :, rows - edge :]),
        pack(load[:HALO], classes[:, :, :edge]),
        "grp",
    )
    west, west_class = unpack(from_w, strip_w, classes[:, :edge])
    east, east_class_x = unpack(from_e, strip_w, classes[:, :edge])
    north, north_class_x = unpack(from_n, load[:HALO], classes[:, :, :edge])
    south, south_class_x = unpack(from_s, load[:HALO], classes[:, :, :edge])

    def corner_load(first):
        return jnp.stack(
            [jnp.swapaxes(x[:, first : first + HALO], 0, 1) for x in (north, south)]
        )

    def corner_class(first):
        return jnp.stack([x[:, first : first + edge] for x in (north_class_x, south_class_x)])

    corner_w, corner_e = exchange(
        pack(corner_load(cols - HALO), corner_class(cols - edge)),
        pack(corner_load(0), corner_class(0)),
        "dev",
    )
    cw, cw_class = unpack(corner_w, corner_load(0), corner_class(0))
    ce, ce_class = unpack(corner_e, corner_load(0), corner_class(0))
    corners = jnp.stack([cw, ce]).reshape(2, 2, HALO * HALO, LANES)
    whole = jnp.concatenate(
        [
            jnp.concatenate([cw_class[0], north_class_x, ce_class[0]], axis=1),
            jnp.concatenate([west_class, classes, east_class_x], axis=1),
            jnp.concatenate([cw_class[1], south_class_x, ce_class[1]], axis=1),
        ],
        axis=2,
    )
    side = PAD - edge
    whole = jnp.pad(whole, ((0, 0), (side, side), (0, 0)))
    cond = jnp.zeros_like(whole)
    for k in range(cond_table.shape[0]):
        cond = jnp.where(whole == k, cond_table[k], cond)
    col_ids = (col_start - PAD + jnp.arange(cols + 2 * PAD))[:, None]
    row_ids = (row_start - edge + jnp.arange(rows + 2 * edge))[None]
    in_cols = (col_ids >= 0) & (col_ids < all_cols)
    in_rows = (row_ids >= 0) & (row_ids < all_rows)
    inside = in_cols & in_rows
    near = (jnp.abs(jnp.arange(cols + 2 * PAD) * 2 - (cols + 2 * PAD - 1)) < cols + 2 * edge)[:, None]
    inside = inside & near
    east0 = jnp.where(inside & (row_ids < all_rows - 1), cond[0], 0.0)
    north0 = jnp.where(inside & (col_ids < all_cols - 1), cond[1], 0.0)
    ext_rows = -(-(rows + 2 * HALO) // GROUP) * GROUP
    grow = ext_rows + 1 - (rows + 2 * edge)

    def fit(x):
        return jnp.pad(x, ((0, 0), (0, grow))) if grow >= 0 else x[:, :grow]

    coef0 = stencil_coefs(fit(east0), fit(north0), SHUNT_CONDUCT)

    half_rows, half_cols = rows // 2, cols // 2
    wide1 = half_cols + HALO - 2
    rows1 = -(-(half_rows + 16) // GROUP) * GROUP
    dot = functools.partial(jnp.dot, precision=HIGH)

    def lead(count, half, first, odd):
        return pair_matrix(count, half, first, odd)

    c_first = PAD - (HALO - 2)
    n0c, n0r = cols + 2 * PAD, rows + 2 * edge
    r_first = edge - 14
    sum_c = lead(n0c, wide1, c_first, False).T
    odd_c = lead(n0c, wide1, c_first, True).T
    sum_r = lead(n0r, rows1 + 1, r_first, False)
    odd_r = lead(n0r, rows1 + 1, r_first, True)
    east1 = dot(dot(sum_c, east0), odd_r)
    north1 = dot(dot(odd_c, north0), sum_r)
    coef1 = stencil_coefs(east1, north1, SHUNT_CONDUCT * 4.0)

    q_rows, q_cols = rows // 4, cols // 4
    east2 = dot(dot(pair_matrix(wide1, q_cols, 4).T, east1), pair_matrix(rows1 + 1, q_rows, 7, True))
    north2 = dot(
        dot(pair_matrix(wide1, q_cols, 4, True).T, north1), pair_matrix(rows1 + 1, q_rows, 7)
    )
    mine = jnp.stack([east2, north2]).reshape(1, -1, LANES)
    spread_out = jnp.broadcast_to(mine, (nd,) + mine.shape[1:])
    gathered = lax.all_to_all(spread_out, AXES, split_axis=0, concat_axis=0, tiled=True)
    cond2 = gathered.reshape(ng, nd_axis, 2, q_cols, q_rows)
    cond2 = cond2.transpose(2, 1, 3, 0, 4).reshape(2, nd_axis * q_cols, ng * q_rows)

    tap_count, tap_code, tap_amps = live_taps(
        taps, tap_current, rows, cols, row_start, col_start, all_cols
    )
    wide0 = cols + 2 * PAD
    s2_rows = rows1 // 2 * q_cols
    slab_rows = pc * q_rows * q_cols // LANES
    s0, p0, s1, p1, slab = pl.pallas_call(
        functools.partial(down_kernel, dims),
        out_shape=[
            shape(ext_rows, wide0, LANES),
            shape(ext_rows + 2, wide0, LANES),
            shape(rows1, wide1, LANES),
            shape(rows1 + 2, wide1, LANES),
            shape(nd * slab_rows, LANES),
        ],
        in_specs=[SMEM] * 3 + [VMEM] * 8,
        out_specs=[VMEM] * 5,
        scratch_shapes=[
            vmem(ext_rows + 2, wide0, LANES),
            vmem(rows1 + 2, wide1, LANES),
            vmem(s2_rows, LANES),
            vmem(GROUP // 2, wide0, LANES),
            vmem(GROUP // 2, wide1, LANES),
        ],
        compiler_params=PARAMS,
        name="fine_down",
    )(tap_count, tap_code, tap_amps, load, west, east, north, south, corners, coef0, coef1)

    got = lax.all_to_all(
        slab.reshape(nd, slab_rows, LANES), AXES, split_axis=0, concat_axis=0, tiled=True
    )
    per = LANES // q_rows
    source2 = got.reshape(ng, nd_axis, q_cols // per, pc, per, q_rows)
    source2 = source2.transpose(3, 1, 4, 2, 0, 5).reshape(pc, nd_axis * q_cols, ng * q_rows)

    fix = coarse_cycle(source2, cond2[0], cond2[1], 2)

    padded = jnp.pad(fix, ((0, 0), (2, 2), (2, LANES)))
    pieces = [
        padded[:, d * q_cols : d * q_cols + q_cols + 4, g * q_rows : g * q_rows + LANES]
        for g in range(ng)
        for d in range(nd_axis)
    ]
    back = jnp.stack(pieces).transpose(0, 2, 1, 3).reshape(nd, (q_cols + 4) * pc, LANES)
    back = lax.all_to_all(back, AXES, split_axis=0, concat_axis=0, tiled=True)
    pitch2 = -(-(q_cols + 4) // GROUP) * GROUP
    return pl.pallas_call(
        functools.partial(up_kernel, dims),
        out_shape=shape(rows, cols, LANES),
        in_specs=[VMEM] * 7,
        out_specs=VMEM,
        scratch_shapes=[
            vmem((q_rows + 4) * pitch2, LANES),
            vmem(rows1 + 2, wide1, LANES),
            vmem(rows1 + 2, wide1, LANES),
            vmem(2 * wide1, LANES),
            vmem(ext_rows + 2, 2 * wide1, LANES),
            vmem(ext_rows + 2, 2 * wide1, LANES),
        ],
        compiler_params=PARAMS,
        name="fine_up",
    )(back.reshape(-1, LANES), s0, p0, s1, p1, coef0, coef1)


def solution(mesh):
    return jax.shard_map(
        body,
        mesh=mesh,
        in_specs=(P("grp", "dev", None), P("grp", "dev"), P("grp", "dev"), P(), P(), P()),
        out_specs=P("grp", "dev", None),
        check_vma=False,
    )
```

```python
import functools

import jax
import jax.numpy as jnp
from jax import lax
from jax.experimental import pallas as pl
from jax.experimental.pallas import tpu as pltpu
from jax.sharding import PartitionSpec as P

LEVELS = 5
RELAXATION = 0.8
KEEP = 1.0 - RELAXATION
SHUNT_CONDUCT = 0.01
AXES = ("grp", "dev")
HIGH = lax.Precision.HIGHEST

HALO = 10
PAD = 12
ROW_PAD = 16
LANES = 128
GROUP = 8


def exchange(tail, head, axis):
    count = lax.axis_size(axis)
    up = [(i, i + 1) for i in range(count - 1)]
    down = [(i + 1, i) for i in range(count - 1)]
    return lax.ppermute(tail, axis, up), lax.ppermute(head, axis, down)


def pack(rows, extra):
    flat = extra.reshape(-1)
    size = -flat.shape[0] % LANES
    return jnp.concatenate([rows.reshape(-1, LANES), jnp.pad(flat, (0, size)).reshape(-1, LANES)])


def unpack(packed, rows, extra):
    count = rows.size // LANES
    flat = packed[count:].reshape(-1)[: extra.size]
    return packed[:count].reshape(rows.shape), flat.reshape(extra.shape)


def pair_matrix(count, half, first=0, odd_only=False):
    fine = jnp.arange(count)[:, None] - first
    coarse = jnp.arange(half)[None, :]
    hit = fine == 2 * coarse + 1 if odd_only else fine // 2 == coarse
    return hit.astype(jnp.float32)


def stencil_coefs(east, north, shunt):
    west = east[:, :-1]
    east = east[:, 1:]
    north = north[:, 1:]
    south = jnp.pad(north, ((1, 0), (0, 0)))[:-1]
    diag = shunt + east + west + north + south
    coefs = jnp.stack([east, north, RELAXATION / diag])
    rows = coefs.shape[2]
    tiles = -(-rows // LANES)
    coefs = jnp.pad(coefs, ((0, 0), (0, 0), (0, tiles * LANES - rows)))
    return jnp.moveaxis(coefs.reshape(3, coefs.shape[1], tiles, LANES), 2, 1)


RING = 4 * GROUP


def wave(groups, stop, width, coef, coef_first, shunt, rings, fill, source, middle, finish):
    ring_e, ring_n, ring_w, ring_a, ring_b, flux_b, again_b, flux_c, turn = rings
    low, high = groups
    per_tile = LANES // GROUP
    for ref in rings:
        ref[...] = jnp.zeros_like(ref)

    def at(ref, row, ahead=0):
        base = pl.multiple_of(lax.rem(row, RING) * width, GROUP)
        return ref[pl.ds(base + ahead, width), :]

    def put(ref, row, value):
        base = pl.multiple_of(lax.rem(row, RING) * width, GROUP)
        ref[pl.ds(base, width), :] = value

    def balance(ring, row, before, slot):
        here = at(ring, row)
        east = at(ring_e, row) * (at(ring, row + 1) - here)
        north = at(ring_n, row) * (at(ring, row, 1) - here)
        turn[slot, pl.ds(GROUP, width), :] = north
        south = turn[slot, pl.ds(GROUP - 1, width), :]
        total = (east - before) + (north - south) + (source(row) - shunt * here)
        return here, east, total

    def go(t, carry):
        g = jnp.minimum(t, high - 1)
        shift = lax.rem(LANES - lax.rem(g, per_tile) * GROUP, LANES)
        found = [
            pltpu.roll(coef[k, g // per_tile, pl.ds(coef_first, width), :], shift, 1)
            for k in range(3)
        ]
        for r in range(GROUP):
            row = g * GROUP + r
            east, north, weight = (
                jnp.broadcast_to(x[:, r : r + 1], (width, LANES)) for x in found
            )
            put(ring_e, row, east)
            put(ring_n, row, north)
            put(ring_w, row, weight)
            put(ring_a, row, fill(r, row, weight))
        g = jnp.clip(t - 1, low, high - 1)
        flux = jnp.where(t > high, again_b[...], flux_b[...])
        again_b[...] = flux
        for r in range(GROUP):
            row = g * GROUP + r
            here, flux, total = balance(ring_a, row, flux, r)
            value = here + at(ring_w, row) * total
            put(ring_b, row, value)
            middle(row, value)
        flux_b[...] = flux
        g = jnp.clip(t - 2, low, high - 1)
        flux = flux_c[...]
        for r in range(GROUP):
            row = g * GROUP + r
            here, flux, total = balance(ring_b, row, flux, GROUP + r)
            finish(g, r, row, here, total, lambda row=row: at(ring_w, row))
        flux_c[...] = flux
        return carry

    lax.fori_loop(low, stop + 2, go, 0)


def rings_for(width):
    ring = vmem(RING * width + GROUP, LANES)
    return [ring] * 5 + [vmem(width, LANES)] * 3 + [vmem(2 * GROUP, width + GROUP, LANES)]


def down_kernel(
    dims, shunts, tap_count, tap_code, tap_amps, own, west, east, north, south, corners,
    coef0, coef1, s0, p0, s1, p1, slab, s2, pair, pair1, *rings,
):
    rows, cols, nd, pc = dims
    wide = cols + 2 * PAD
    ext = s0.shape[0] // wide
    rings0, rings1 = rings[:9], rings[9:]

    s0[...] = jnp.zeros_like(s0)
    first = ROW_PAD - HALO

    def copy_own(i, carry):
        s0[pl.ds((i + ROW_PAD) * wide + PAD, cols), :] = -own[i]
        return carry

    lax.fori_loop(0, rows, copy_own, 0, unroll=8)
    for i in range(HALO):
        s0[pl.ds((first + i) * wide + PAD, cols), :] = -north[i]
        s0[pl.ds((ROW_PAD + rows + i) * wide + PAD, cols), :] = -south[i]
    for j in range(HALO):
        for side, (strip, col) in enumerate(((west, PAD - HALO), (east, PAD + cols))):
            s0[pl.ds(ROW_PAD * wide + col + j, rows, stride=wide), :] = -strip[j]
            for end, base in enumerate((first, ROW_PAD + rows)):
                block = corners[side, end, j * HALO : (j + 1) * HALO, :]
                s0[pl.ds(base * wide + col + j, HALO, stride=wide), :] = -block

    lane = lax.broadcasted_iota(jnp.int32, (GROUP, LANES), 1)
    sub = lax.broadcasted_iota(jnp.int32, (GROUP, LANES), 0)

    def add_tap(k, carry):
        code = tap_code[k]
        node = code // LANES
        base = pl.multiple_of(node // GROUP * GROUP, GROUP)
        hit = (lane == lax.rem(code, LANES)) & (sub == node - base)
        s0[pl.ds(base, GROUP), :] += jnp.where(hit, tap_amps[k], 0.0)
        return carry

    lax.fori_loop(0, tap_count[0], add_tap, 0)

    def smooth_and_restrict(source, pre, coef, shunt, pair, rings, store):
        width = pair.shape[1]
        held = []

        def row_of(ref, row):
            return ref[pl.ds(pl.multiple_of(row * width, GROUP), width), :]

        def middle(row, value):
            pre[pl.ds(pl.multiple_of(row * width, GROUP), width), :] = value

        def finish(g, r, row, here, total, weight):
            if r % 2 == 0:
                held.append(total)
            else:
                pair[r // 2] = held.pop() + total
                store(g * (GROUP // 2) + r // 2, r // 2)

        groups = source.shape[0] // width // GROUP
        wave(
            (0, groups), groups - 1, width, coef, 0, shunt, rings,
            lambda r, row, weight: weight * row_of(source, row),
            lambda row: row_of(source, row), middle, finish,
        )

    half = pair1.shape[1]
    start = PAD - (HALO - 2)

    def store1(k, m):
        s1[pl.ds(pl.multiple_of(k * half, GROUP), half), :] = (
            pair[m, pl.ds(start, half, stride=2), :] + pair[m, pl.ds(start + 1, half, stride=2), :]
        )

    smooth_and_restrict(s0, p0, coef0, shunts[0], pair, rings0, store1)
    quarter = cols // 4

    def store2(k, m):
        s2[pl.ds(pl.multiple_of(k * quarter, quarter), quarter), :] = (
            pair1[m, pl.ds(4, quarter, stride=2), :] + pair1[m, pl.ds(5, quarter, stride=2), :]
        )

    smooth_and_restrict(s1, p1, coef1, shunts[1], pair1, rings1, store2)
    rows2 = rows // 4
    per = LANES // rows2
    groups = quarter // per
    for jp in range(groups):
        parts = [
            s2[pl.ds(ROW_PAD // 4 * quarter + jl * groups + jp, rows2, stride=quarter), :]
            for jl in range(per)
        ]
        turned = jnp.concatenate(parts, axis=0).T
        for p in range(pc):
            slab[pl.ds(jp * pc + p, nd, stride=groups * pc), :] = turned[p * nd : (p + 1) * nd]


def up_kernel(dims, shunts, back, s0, p0, s1, p1, coef0, coef1, out, x2, c1, twice1, twice0, *rings):
    rows, cols, nd, pc = dims
    wide = cols + 2 * PAD
    quarter = cols // 4
    wide2 = quarter + 4
    width1 = 2 * wide2
    width0 = 2 * width1
    rows2 = rows // 4 + 4
    pitch2 = x2.shape[0] // rows2
    rings0, rings1 = rings[:9], rings[9:]
    for jw in range(wide2):
        parts = [back[pl.ds(jw * pc + p, nd, stride=wide2 * pc), :] for p in range(pc)]
        turned = jnp.concatenate(parts, axis=0).T
        x2[pl.ds(jw, rows2, stride=pitch2), :] = turned[:rows2]

    def lifted(twice, slot, x):
        count = x.shape[0]
        twice[slot, pl.ds(0, count, stride=2), :] = x
        twice[slot, pl.ds(1, count, stride=2), :] = x
        return twice[slot]

    def fill1(r, row, weight):
        k = jnp.clip(row // 2 - 2, 0, rows2 - 1)
        x = x2[pl.ds(pl.multiple_of(k * pitch2, GROUP), pitch2), :][:wide2]
        return p1[pl.ds(pl.multiple_of(row * width1, GROUP), width1), :] + lifted(
            twice1, r, x
        )

    def source1(row):
        return s1[pl.ds(pl.multiple_of(row * width1, GROUP), width1), :]

    def finish1(g, r, row, here, total, weight):
        c1[pl.ds(pl.multiple_of(row * width1, GROUP), width1), :] = here + weight() * total

    groups1 = s1.shape[0] // width1 // GROUP
    wave(
        (0, groups1), groups1, width1, coef1, 0, shunts[1], rings1,
        fill1, source1, lambda row, value: None, finish1,
    )

    start = PAD - (HALO - 2)

    def fill0(r, row, weight):
        x = c1[pl.ds(pl.multiple_of(row // 2 * width1, GROUP), width1), :]
        return p0[pl.ds(row * wide + start, width0), :] + lifted(twice0, r, x)

    def source0(row):
        return s0[pl.ds(row * wide + start, width0), :]

    first, last = ROW_PAD // GROUP, (ROW_PAD + rows) // GROUP

    def finish0(g, r, row, here, total, weight):
        done = here + weight() * total
        row = jnp.clip(row - ROW_PAD, r, rows - GROUP + r)
        out[row] = done[HALO - 2 : HALO - 2 + cols]

    wave(
        (first - 1, last + 1), last, width0, coef0, start, shunts[0], rings0,
        fill0, source0, lambda row, value: None, finish0,
    )


VMEM = pl.BlockSpec(memory_space=pltpu.VMEM)
SMEM = pl.BlockSpec(memory_space=pltpu.SMEM)
PARAMS = pltpu.CompilerParams(vmem_limit_bytes=40 * 2**20)


SMALL = pltpu.CompilerParams(vmem_limit_bytes=16 * 2**20)


def shape(*dims):
    return jax.ShapeDtypeStruct(dims, jnp.float32)


def vmem(*dims):
    return pltpu.VMEM(dims, jnp.float32)


def lane_chunks(x):
    return [x[:, i : i + LANES] for i in range(0, x.shape[1], LANES)]


def block_column(x, k):
    size = x.shape[0]
    lane = lax.broadcasted_iota(jnp.int32, (size, LANES), 1)
    at = lane // size * size + k
    take = functools.partial(jnp.take_along_axis, axis=1, mode="promise_in_bounds")
    return jnp.concatenate([take(c, at) for c in lane_chunks(x)], axis=1)


def block_rows(held, x):
    held[...] = x

    def row(k):
        return jnp.broadcast_to(held[pl.ds(k, 1), :], x.shape)

    return row


def over(size, step, start):
    return lax.fori_loop(0, size, step, start, unroll=size <= GROUP)


def block_product(held, x, *others):
    rows = [block_rows(h, y) for h, y in zip(held, others)]

    def step(k, totals):
        column = block_column(x, k)
        return tuple(t + column * row(k) for t, row in zip(totals, rows))

    return over(x.shape[0], step, tuple(jnp.zeros_like(x) for _ in others))


def block_inverse(held, x):
    size, count = x.shape
    inner = lax.broadcasted_iota(jnp.int32, x.shape, 1) % size
    row_id = lax.broadcasted_iota(jnp.int32, x.shape, 0)

    def step(k, x):
        row = block_rows(held[0], x)(k)
        column = block_column(x, k)
        pivot = block_rows(held[1], column)(k)
        scaled = jnp.where(inner == k, 1.0, row) / pivot
        rest = jnp.where(inner == k, 0.0, x) - column * scaled
        return jnp.where(row_id == k, scaled, rest)

    return over(size, step, x)


def ahead(x, blocks):
    lanes = x.shape[1]
    return pltpu.roll(x, (-blocks * x.shape[0]) % lanes, 1)


def factor_kernel(diag, right, parts, last, *held):
    size, count = diag.shape
    d, c, ct = diag[...], right[...], right[...]
    stride = 1
    level = 0
    while stride * size < count:
        inverse = block_inverse(held, d)
        (r,) = block_product(held, c, ahead(inverse, stride))
        (lx,) = block_product(held, ct, inverse)
        left, lead = ahead(lx, -stride), ahead(lx, stride)
        for i, part in enumerate((r, left, inverse, c, ahead(ct, -stride))):
            parts[level, i] = part
        first, new_c = block_product(held, r, ct, ahead(c, stride))
        (second,) = block_product(held, left, ahead(c, -stride))
        (new_ct,) = block_product(held, lead, ct)
        d = d - first - second
        c, ct = -new_c, -new_ct
        stride *= 2
        level += 1
    last[...] = block_inverse(held, d)


def solve_kernel(source, parts, last, out, *held):
    size, count = source.shape
    block = lax.broadcasted_iota(jnp.int32, source.shape, 1) // size
    f = source[...]
    levels = parts.shape[0]
    for level in range(levels):
        s = 2**level
        (a,) = block_product(held, parts[level, 0], ahead(f, s))
        (b,) = block_product(held, parts[level, 1], ahead(f, -s))
        f = jnp.where(block % (2 * s) == 0, f - a - b, f)
    (x,) = block_product(held, last[...], f)
    for level in reversed(range(levels)):
        s = 2**level
        (a,) = block_product(held, parts[level, 3], ahead(x, s))
        (b,) = block_product(held, parts[level, 4], ahead(x, -s))
        (new,) = block_product(held, parts[level, 2], f - a - b)
        x = jnp.where(block % (2 * s) == s, new, x)
    out[...] = x


def coarse_factor(east, north, shunt):
    size, blocks = east.shape
    west = jnp.pad(east, ((0, 0), (1, 0)))[:, :-1]
    south = jnp.pad(north, ((1, 0), (0, 0)))[:-1]
    diag = shunt + east + west + north + south
    row, col = jnp.arange(size)[:, None, None], jnp.arange(size)[None, None, :]
    flat = (size, blocks * size)
    main = jnp.where(row == col, diag[:, :, None], 0.0)
    main = main - jnp.where(col == row + 1, north[:, :, None], 0.0)
    main = (main - jnp.where(col == row - 1, south[:, :, None], 0.0)).reshape(flat)
    right = jnp.where(row == col, -east[:, :, None], 0.0).reshape(flat)
    levels = blocks.bit_length() - 1
    return pl.pallas_call(
        factor_kernel,
        out_shape=[shape(levels, 5, *flat), shape(*flat)],
        in_specs=[VMEM] * 2,
        out_specs=[VMEM] * 2,
        scratch_shapes=[vmem(*flat)] * 2,
        compiler_params=SMALL,
        name="coarse_factor",
    )(main, right)


def coarse_solve(source, factor):
    cands, size, blocks = source.shape
    flat = (size, blocks * size)
    laid = jnp.pad(source.transpose(1, 2, 0), ((0, 0), (0, 0), (0, size - cands))).reshape(flat)
    solved = pl.pallas_call(
        solve_kernel,
        out_shape=shape(*flat),
        in_specs=[VMEM] * 3,
        out_specs=VMEM,
        scratch_shapes=[vmem(*flat)] * 2,
        compiler_params=SMALL,
        name="coarse_solve",
    )(laid, *factor)
    return solved.reshape(size, blocks, size)[:, :, :cands].transpose(2, 0, 1)


def operate_lead(v, east, north, shunt):
    padded = jnp.pad(v, ((0, 0), (1, 1), (1, 1)))
    west = jnp.pad(east, ((0, 0), (1, 0)))[:, :-1]
    south = jnp.pad(north, ((1, 0), (0, 0)))[:-1]
    diag = shunt + east + west + north + south
    applied = (
        diag * v
        - east * padded[:, 1:-1, 2:]
        - west * padded[:, 1:-1, :-2]
        - north * padded[:, 2:, 1:-1]
        - south * padded[:, :-2, 1:-1]
    )
    return applied, diag


def relax_lead(v, source, east, north, shunt):
    applied, diag = operate_lead(v, east, north, shunt)
    return v + RELAXATION * (source - applied) / diag


def coarse_levels(east, north, level):
    dot = functools.partial(jnp.dot, precision=HIGH)
    levels = []
    while level < LEVELS:
        nj, ni = east.shape
        levels.append((east, north))
        pi, pj = pair_matrix(ni, ni // 2), pair_matrix(nj, nj // 2)
        odd_i = pair_matrix(ni, ni // 2, odd_only=True)
        odd_j = pair_matrix(nj, nj // 2, odd_only=True)
        east, north = dot(pj.T, dot(east, odd_i)), dot(odd_j.T, dot(north, pi))
        level += 1
    return levels, coarse_factor(east, north, SHUNT_CONDUCT * 4.0**LEVELS)


def coarse_cycle(source, levels, factor, level):
    if level == LEVELS:
        return coarse_solve(source, factor)
    shunt = SHUNT_CONDUCT * 4.0**level
    east, north = levels[0]
    count, nj, ni = source.shape
    _, diag = operate_lead(source, east, north, shunt)
    pre = relax_lead(RELAXATION * source / diag, source, east, north, shunt)
    rest = source - operate_lead(pre, east, north, shunt)[0]
    pi = pair_matrix(ni, ni // 2)
    pj = pair_matrix(nj, nj // 2)
    dot = functools.partial(jnp.einsum, precision=HIGH)
    coarse = dot("pji,jJ,iI->pJI", rest, pj, pi)
    fix = coarse_cycle(coarse, levels[1:], factor, level + 1)
    v = pre + dot("pJI,jJ,iI->pji", fix, pj, pi)
    v = relax_lead(v, source, east, north, shunt)
    return relax_lead(v, source, east, north, shunt)


def live_taps(taps, tap_current, rows, cols, row_start, col_start, all_cols):
    i = taps // all_cols - row_start
    j = taps % all_cols - col_start
    inside = (i >= -HALO) & (i < rows + HALO) & (j >= -HALO) & (j < cols + HALO)
    cand = lax.broadcasted_iota(jnp.int32, taps.shape, 0)
    code = ((i + ROW_PAD) * (cols + 2 * PAD) + j + PAD) * LANES + cand
    count = taps.size
    lead = count // LANES
    flags = inside.reshape(lead, LANES).astype(jnp.float32)
    upto = jnp.dot(flags, jnp.triu(jnp.ones((LANES, LANES), jnp.float32)), precision=HIGH)
    before = jnp.dot(
        jnp.tril(jnp.ones((lead, lead), jnp.float32), -1), upto[:, -1:], precision=HIGH
    )
    place = (upto + before).astype(jnp.int32).reshape(-1)
    place = jnp.where(inside.reshape(-1), place - 1, -1)
    pick = place[None, :] == jnp.arange(count, dtype=jnp.int32)[:, None]
    codes = jnp.sum(jnp.where(pick, code.reshape(-1)[None], 0), axis=1)
    amps = jnp.sum(jnp.where(pick, tap_current.reshape(-1)[None], 0.0), axis=1)
    return jnp.sum(inside.astype(jnp.int32)).reshape(1), codes, amps


def body(load, east_class, north_class, cond_table, taps, tap_current):
    rows, cols, cands = load.shape
    ng, nd_axis = lax.axis_size("grp"), lax.axis_size("dev")
    nd = ng * nd_axis
    pc = cands // nd
    row_start = lax.axis_index("grp") * rows
    col_start = lax.axis_index("dev") * cols
    all_rows, all_cols = ng * rows, nd_axis * cols
    edge = HALO + 1
    dims = (rows, cols, nd, pc)

    classes = jnp.stack([east_class.T, north_class.T]).astype(jnp.float32)
    strip_w = jnp.swapaxes(load[:, :HALO], 0, 1)
    strip_e = jnp.swapaxes(load[:, cols - HALO :], 0, 1)
    from_w, from_e = exchange(
        pack(strip_e, classes[:, cols - edge :]), pack(strip_w, classes[:, :edge]), "dev"
    )
    from_n, from_s = exchange(
        pack(load[rows - HALO :], classes[:, :, rows - edge :]),
        pack(load[:HALO], classes[:, :, :edge]),
        "grp",
    )
    west, west_class = unpack(from_w, strip_w, classes[:, :edge])
    east, east_class_x = unpack(from_e, strip_w, classes[:, :edge])
    north, north_class_x = unpack(from_n, load[:HALO], classes[:, :, :edge])
    south, south_class_x = unpack(from_s, load[:HALO], classes[:, :, :edge])

    def corner_load(first):
        return jnp.stack(
            [jnp.swapaxes(x[:, first : first + HALO], 0, 1) for x in (north, south)]
        )

    def corner_class(first):
        return jnp.stack([x[:, first : first + edge] for x in (north_class_x, south_class_x)])

    corner_w, corner_e = exchange(
        pack(corner_load(cols - HALO), corner_class(cols - edge)),
        pack(corner_load(0), corner_class(0)),
        "dev",
    )
    cw, cw_class = unpack(corner_w, corner_load(0), corner_class(0))
    ce, ce_class = unpack(corner_e, corner_load(0), corner_class(0))
    corners = jnp.stack([cw, ce]).reshape(2, 2, HALO * HALO, LANES)
    whole = jnp.concatenate(
        [
            jnp.concatenate([cw_class[0], north_class_x, ce_class[0]], axis=1),
            jnp.concatenate([west_class, classes, east_class_x], axis=1),
            jnp.concatenate([cw_class[1], south_class_x, ce_class[1]], axis=1),
        ],
        axis=2,
    )
    side = PAD - edge
    whole = jnp.pad(whole, ((0, 0), (side, side), (0, 0)))
    cond = jnp.zeros_like(whole)
    for k in range(cond_table.shape[0]):
        cond = jnp.where(whole == k, cond_table[k], cond)
    col_ids = (col_start - PAD + jnp.arange(cols + 2 * PAD))[:, None]
    row_ids = (row_start - edge + jnp.arange(rows + 2 * edge))[None]
    in_cols = (col_ids >= 0) & (col_ids < all_cols)
    in_rows = (row_ids >= 0) & (row_ids < all_rows)
    inside = in_cols & in_rows
    near = (jnp.abs(jnp.arange(cols + 2 * PAD) * 2 - (cols + 2 * PAD - 1)) < cols + 2 * edge)[:, None]
    inside = inside & near
    east0 = jnp.where(inside & (row_ids < all_rows - 1), cond[0], 0.0)
    north0 = jnp.where(inside & (col_ids < all_cols - 1), cond[1], 0.0)
    wide0 = cols + 2 * PAD
    ext_rows = rows + 2 * ROW_PAD
    grow = ROW_PAD + 1 - edge
    fit = ((0, 0), (grow, ROW_PAD - edge))
    coef0 = stencil_coefs(jnp.pad(east0, fit), jnp.pad(north0, fit), SHUNT_CONDUCT)

    half_rows, half_cols = rows // 2, cols // 2
    wide1 = half_cols + HALO - 2
    rows1 = half_rows + ROW_PAD
    dot = functools.partial(jnp.dot, precision=HIGH)
    c_first = PAD - (HALO - 2)
    n0r = rows + 2 * edge
    r_first = edge - ROW_PAD - 2
    sum_c = pair_matrix(wide0, wide1, c_first).T
    odd_c = pair_matrix(wide0, wide1, c_first, True).T
    sum_r = pair_matrix(n0r, rows1 + 1, r_first)
    odd_r = pair_matrix(n0r, rows1 + 1, r_first, True)
    east1 = dot(dot(sum_c, east0), odd_r)
    north1 = dot(dot(odd_c, north0), sum_r)
    coef1 = stencil_coefs(east1, north1, SHUNT_CONDUCT * 4.0)

    q_rows, q_cols = rows // 4, cols // 4
    east2 = dot(dot(pair_matrix(wide1, q_cols, 4).T, east1), pair_matrix(rows1 + 1, q_rows, 9, True))
    north2 = dot(
        dot(pair_matrix(wide1, q_cols, 4, True).T, north1), pair_matrix(rows1 + 1, q_rows, 9)
    )
    mine = jnp.stack([east2, north2]).reshape(1, -1, LANES)
    spread_out = jnp.broadcast_to(mine, (nd,) + mine.shape[1:])
    gathered = lax.all_to_all(spread_out, AXES, split_axis=0, concat_axis=0, tiled=True)
    cond2 = gathered.reshape(ng, nd_axis, 2, q_cols, q_rows)
    cond2 = cond2.transpose(2, 1, 3, 0, 4).reshape(2, nd_axis * q_cols, ng * q_rows)

    levels, factor = coarse_levels(cond2[0], cond2[1], 2)

    tap_count, tap_code, tap_amps = live_taps(
        taps, tap_current, rows, cols, row_start, col_start, all_cols
    )
    s2_rows = rows1 // 2 * q_cols
    slab_rows = pc * q_rows * q_cols // LANES
    shunts = (SHUNT_CONDUCT, SHUNT_CONDUCT * 4.0)
    s0, p0, s1, p1, slab = pl.pallas_call(
        functools.partial(down_kernel, dims, shunts),
        out_shape=[
            shape(ext_rows * wide0, LANES),
            shape(ext_rows * wide0, LANES),
            shape(rows1 * wide1, LANES),
            shape(rows1 * wide1, LANES),
            shape(nd * slab_rows, LANES),
        ],
        in_specs=[SMEM] * 3 + [VMEM] * 8,
        out_specs=[VMEM] * 5,
        scratch_shapes=[
            vmem(s2_rows, LANES),
            vmem(GROUP // 2, wide0, LANES),
            vmem(GROUP // 2, wide1, LANES),
        ]
        + rings_for(wide0)
        + rings_for(wide1),
        compiler_params=PARAMS,
        name="fine_down",
    )(tap_count, tap_code, tap_amps, load, west, east, north, south, corners, coef0, coef1)

    got = lax.all_to_all(
        slab.reshape(nd, slab_rows, LANES), AXES, split_axis=0, concat_axis=0, tiled=True
    )
    per = LANES // q_rows
    source2 = got.reshape(ng, nd_axis, q_cols // per, pc, per, q_rows)
    source2 = source2.transpose(3, 1, 4, 2, 0, 5).reshape(pc, nd_axis * q_cols, ng * q_rows)

    fix = coarse_cycle(source2, levels, factor, 2)

    padded = jnp.pad(fix, ((0, 0), (2, 2), (2, LANES)))
    pieces = [
        padded[:, d * q_cols : d * q_cols + q_cols + 4, g * q_rows : g * q_rows + LANES]
        for g in range(ng)
        for d in range(nd_axis)
    ]
    back = jnp.stack(pieces).transpose(0, 2, 1, 3).reshape(nd, (q_cols + 4) * pc, LANES)
    back = lax.all_to_all(back, AXES, split_axis=0, concat_axis=0, tiled=True)
    pitch2 = -(-(q_cols + 4) // GROUP) * GROUP
    return pl.pallas_call(
        functools.partial(up_kernel, dims, shunts),
        out_shape=shape(rows, cols, LANES),
        in_specs=[VMEM] * 7,
        out_specs=VMEM,
        scratch_shapes=[
            vmem((q_rows + 4) * pitch2, LANES),
            vmem(rows1 * wide1, LANES),
            vmem(GROUP, wide1, LANES),
            vmem(GROUP, 2 * wide1, LANES),
        ]
        + rings_for(2 * wide1)
        + rings_for(wide1),
        compiler_params=PARAMS,
        name="fine_up",
    )(back.reshape(-1, LANES), s0, p0, s1, p1, coef0, coef1)


def solution(mesh):
    return jax.shard_map(
        body,
        mesh=mesh,
        in_specs=(P("grp", "dev", None), P("grp", "dev"), P("grp", "dev"), P(), P(), P()),
        out_specs=P("grp", "dev", None),
        check_vma=False,
    )
```

```python
import functools

import jax
import jax.numpy as jnp
from jax import lax
from jax.experimental import pallas as pl
from jax.experimental.pallas import tpu as pltpu
from jax.sharding import PartitionSpec as P

LEVELS = 5
RELAXATION = 0.8
KEEP = 1.0 - RELAXATION
SHUNT_CONDUCT = 0.01
AXES = ("grp", "dev")
HIGH = lax.Precision.HIGHEST

HALO = 10
PAD = 12
ROW_PAD = 16
LANES = 128
GROUP = 8


def exchange(tail, head, axis):
    count = lax.axis_size(axis)
    up = [(i, i + 1) for i in range(count - 1)]
    down = [(i + 1, i) for i in range(count - 1)]
    return lax.ppermute(tail, axis, up), lax.ppermute(head, axis, down)


RING = 4 * GROUP


def wave(groups, stop, width, coef, coef_first, shunt, rings, fill, source, middle, finish):
    ring_e, ring_n, ring_w, ring_a, ring_b, flux_b, again_b, flux_c, turn = rings
    low, high = groups
    per_tile = LANES // GROUP
    for ref in rings:
        ref[...] = jnp.zeros_like(ref)

    def at(ref, row, ahead=0):
        base = pl.multiple_of(lax.rem(row, RING) * width, GROUP)
        return ref[pl.ds(base + ahead, width), :]

    def put(ref, row, value):
        base = pl.multiple_of(lax.rem(row, RING) * width, GROUP)
        ref[pl.ds(base, width), :] = value

    def balance(ring, row, before, slot):
        here = at(ring, row)
        east = at(ring_e, row) * (at(ring, row + 1) - here)
        north = at(ring_n, row) * (at(ring, row, 1) - here)
        turn[slot, pl.ds(GROUP, width), :] = north
        south = turn[slot, pl.ds(GROUP - 1, width), :]
        total = (east - before) + (north - south) + (source(row) - shunt * here)
        return here, east, total

    def go(t, carry):
        g = jnp.minimum(t, high - 1)
        shift = lax.rem(LANES - lax.rem(g, per_tile) * GROUP, LANES)
        found = [
            pltpu.roll(coef[k, g // per_tile, pl.ds(coef_first, width), :], shift, 1)
            for k in range(3)
        ]
        for r in range(GROUP):
            row = g * GROUP + r
            east, north, weight = (
                jnp.broadcast_to(x[:, r : r + 1], (width, LANES)) for x in found
            )
            put(ring_e, row, east)
            put(ring_n, row, north)
            put(ring_w, row, weight)
            put(ring_a, row, fill(r, row, weight))
        g = jnp.clip(t - 1, low, high - 1)
        flux = jnp.where(t > high, again_b[...], flux_b[...])
        again_b[...] = flux
        for r in range(GROUP):
            row = g * GROUP + r
            here, flux, total = balance(ring_a, row, flux, r)
            value = here + at(ring_w, row) * total
            put(ring_b, row, value)
            middle(row, value)
        flux_b[...] = flux
        g = jnp.clip(t - 2, low, high - 1)
        flux = flux_c[...]
        for r in range(GROUP):
            row = g * GROUP + r
            here, flux, total = balance(ring_b, row, flux, GROUP + r)
            finish(g, r, row, here, total, lambda row=row: at(ring_w, row))
        flux_c[...] = flux
        return carry

    lax.fori_loop(low, stop + 2, go, 0)


def rings_for(width):
    ring = vmem(RING * width + GROUP, LANES)
    return [ring] * 5 + [vmem(width, LANES)] * 3 + [vmem(2 * GROUP, width + GROUP, LANES)]


def strip_kernel(
    dims, place, table, load, east_class, north_class,
    strip_e, strip_w, strip_n, strip_s, cond, shares, held,
):
    rows, cols, nd, pc = dims
    edge = HALO + 1

    def copy(i, carry):
        strip_e[pl.ds(i * HALO, HALO), :] = load[i, cols - HALO :, :]
        strip_w[pl.ds(i * HALO, HALO), :] = load[i, :HALO, :]
        return carry

    lax.fori_loop(0, rows, copy, 0, unroll=8)
    for i in range(HALO):
        strip_n[pl.ds(i * cols, cols), :] = load[rows - HALO + i]
        strip_s[pl.ds(i * cols, cols), :] = load[i]
    coarse = []
    for k, classes in enumerate((east_class, north_class)):
        kind = classes[...]
        value = jnp.zeros(kind.shape, jnp.float32)
        for c in range(table.shape[0]):
            value = jnp.where(kind == c, table[c], value)
        node = lax.broadcasted_iota(jnp.int32, kind.shape, k)
        value = jnp.where(node == place[k], 0.0, value)
        turned = jnp.pad(value, ((0, 0), (0, LANES - cols))).T[:cols]
        cond[k] = turned
        pieces = rows // LANES
        for h in range(pieces):
            at = pl.ds(rows * HALO + k * edge * pieces + h, edge, stride=pieces)
            part = turned[:, h * LANES : (h + 1) * LANES]
            strip_e[at, :] = part[cols - edge :]
            strip_w[at, :] = part[:edge]
        at = pl.ds(cols * HALO + k * cols, cols)
        strip_n[at, :] = pltpu.roll(turned, edge, 1)[:, :LANES]
        strip_s[at, :] = turned[:, :LANES]
        for _ in range(2):
            even, odd = row_pairs(held, turned)
            turned = halve_lanes(even + odd, odd=True) if k == 0 else halve_lanes(odd)
        coarse.append(turned)
    q_rows, q_cols = rows // 4, cols // 4
    per = LANES // q_rows
    group = q_cols // per
    for k, value in enumerate(coarse):
        for jl in range(per):
            shares[pl.ds(k * group, group), pl.ds(jl * q_rows, q_rows)] = value[
                jl * group : (jl + 1) * group, :q_rows
            ]
    mine = shares[pl.ds(0, 2 * group), :]
    for q in range(1, nd):
        shares[pl.ds(q * 2 * group, 2 * group), :] = mine


def corner_kernel(cols, north, south, out_e, out_w):
    edge = HALO + 1
    cond_at = 2 * HALO * HALO
    for ref in (out_e, out_w):
        ref[...] = jnp.zeros_like(ref)
    for end, strip in enumerate((north, south)):
        for i in range(HALO):
            at = pl.ds((end * HALO + i) * HALO, HALO)
            out_e[at, :] = strip[pl.ds((i + 1) * cols - HALO, HALO), :]
            out_w[at, :] = strip[pl.ds(i * cols, HALO), :]
        for k in range(2):
            at = pl.ds(cond_at + (end * 2 + k) * 2 * GROUP, edge)
            first = cols * HALO + k * cols
            out_e[at, :] = strip[pl.ds(first + cols - edge, edge), :]
            out_w[at, :] = strip[pl.ds(first, edge), :]


def coef_kernel(
    dims, cond, west, east, north, south, corner_w, corner_e, coef0, coef1, grid, held
):
    rows, cols, nd, pc = dims
    edge = HALO + 1
    wide0, wide1 = coef0.shape[2], coef1.shape[2]
    pieces = rows // LANES
    first = ROW_PAD - edge
    grids = []
    for k in range(2):
        grid[...] = jnp.zeros_like(grid)
        grid[pl.ds(PAD, cols), pl.ds(ROW_PAD, rows)] = cond[k]
        for strip, col in ((west, PAD - edge), (east, PAD + cols)):
            for h in range(pieces):
                at = pl.ds(rows * HALO + k * edge * pieces + h, edge, stride=pieces)
                grid[pl.ds(col, edge), pl.ds(ROW_PAD + h * LANES, LANES)] = strip[at, :]
        for end, (strip, row) in enumerate(((north, first), (south, ROW_PAD + rows))):
            at = pl.ds(cols * HALO + k * cols, cols)
            grid[pl.ds(PAD, cols), pl.ds(row, edge)] = strip[at, :][:, :edge]
            at = pl.ds(2 * HALO * HALO + (end * 2 + k) * 2 * GROUP, edge)
            for corner, col in ((corner_w, PAD - edge), (corner_e, PAD + cols)):
                grid[pl.ds(col, edge), pl.ds(row, edge)] = corner[at, :][:, :edge]
        grids.append(grid[...])

    def put(coef, east, west, north, south, shunt):
        weight = RELAXATION / (shunt + east + west + north + south)
        for i, value in enumerate((east, north, weight)):
            for t, piece in enumerate(lane_chunks(value)):
                coef[i, t] = piece

    east, north = grids
    put(coef0, east, pltpu.roll(east, 1, 1), north, pltpu.roll(north, 1, 0), SHUNT_CONDUCT)
    tiles = east.shape[1] // LANES

    def picked(start):
        at = pl.ds(start, wide1, stride=2)
        return jnp.concatenate([held[t, at, :] for t in range(tiles)], axis=1)

    start = PAD - (HALO - 2)
    for t, piece in enumerate(lane_chunks(east)):
        held[t] = piece
    east = halve_lanes(picked(start) + picked(start + 1), odd=True)
    for t, piece in enumerate(lane_chunks(north)):
        held[t] = piece
    north, south = halve_lanes(picked(start + 1)), halve_lanes(picked(start - 1))
    put(coef1, east, pltpu.roll(east, 1, 1), north, south, 4.0 * SHUNT_CONDUCT)


def tap_kernel(dims, all_cols, place, taps, currents, count, codes, amps):
    rows, cols, nd, pc = dims

    def turned(x):
        return jnp.pad(x, ((0, 0), (0, LANES - x.shape[1]))).T[: x.shape[1]]

    node = turned(taps[...].astype(jnp.float32)).astype(jnp.int32)
    current = turned(currents[...])
    lead = node.shape[0]
    row_at = node // all_cols
    i = row_at - place[2]
    j = node - row_at * all_cols - place[3]
    inside = (i >= -HALO) & (i < rows + HALO) & (j >= -HALO) & (j < cols + HALO)
    lane = lax.broadcasted_iota(jnp.int32, node.shape, 1)
    code = ((i + ROW_PAD) * (cols + 2 * PAD) + j + PAD) * LANES + lane
    flags = jnp.where(inside, 1.0, 0.0)
    at, to = iota2(LANES, LANES)
    upto = exact_dot(flags, (at <= to).astype(jnp.float32))
    at, to = iota2(lead, lead)
    before = exact_dot((at > to).astype(jnp.float32), upto)[:, LANES - 1 :]
    slot = jnp.where(inside, (upto + before).astype(jnp.int32) - 1, -1)
    total = jnp.sum(flags).astype(jnp.int32)
    count[0] = total
    codes[...] = jnp.zeros_like(codes)
    amps[...] = jnp.zeros_like(amps)
    wanted = lax.broadcasted_iota(jnp.int32, (LANES, LANES), 0)
    code = code.astype(jnp.float32)

    def fill(chunk, carry):
        found = jnp.zeros((LANES, LANES), jnp.float32)
        amount = jnp.zeros((LANES, LANES), jnp.float32)
        for k in range(lead):
            hit = wanted + chunk * LANES == jnp.broadcast_to(slot[k : k + 1], wanted.shape)
            found += jnp.where(hit, jnp.broadcast_to(code[k : k + 1], wanted.shape), 0.0)
            amount += jnp.where(hit, jnp.broadcast_to(current[k : k + 1], wanted.shape), 0.0)
        codes[pl.ds(chunk, 1), :] = jnp.sum(found.T, axis=0, keepdims=True).astype(jnp.int32)
        amps[pl.ds(chunk, 1), :] = jnp.sum(amount.T, axis=0, keepdims=True)
        return carry

    lax.fori_loop(0, (total + LANES - 1) // LANES, fill, 0)


def down_kernel(
    dims, shunts, tap_count, tap_code, tap_amps, own_hbm, west_hbm, east_hbm, north, south,
    corner_w, corner_e, coef0, coef1, s0, p0, s1, p1, slab, own, west, east, sems, s2, pair,
    pair1, *rings,
):
    rows, cols, nd, pc = dims
    wide = cols + 2 * PAD
    ext = s0.shape[0] // wide
    rings0, rings1 = rings[:9], rings[9:]

    moves = [
        pltpu.make_async_copy(source.at[pl.ds(0, here.shape[0])], here, sems.at[k])
        for k, (source, here) in enumerate(((own_hbm, own), (west_hbm, west), (east_hbm, east)))
    ]
    for move in moves:
        move.start()
    s0[...] = jnp.zeros_like(s0)
    for move in moves:
        move.wait()
    first = ROW_PAD - HALO

    def copy_own(i, carry):
        base = (i + ROW_PAD) * wide
        s0[pl.ds(base + PAD, cols), :] = -own[i]
        s0[pl.ds(base + PAD - HALO, HALO), :] = -west[pl.ds(i * HALO, HALO), :]
        s0[pl.ds(base + PAD + cols, HALO), :] = -east[pl.ds(i * HALO, HALO), :]
        return carry

    lax.fori_loop(0, rows, copy_own, 0, unroll=8)
    for k, (strip, base) in enumerate(((north, first), (south, ROW_PAD + rows))):
        for i in range(HALO):
            at = (base + i) * wide + PAD
            corner = pl.ds((k * HALO + i) * HALO, HALO)
            s0[pl.ds(at, cols), :] = -strip[i * cols : (i + 1) * cols, :]
            s0[pl.ds(at - HALO, HALO), :] = -corner_w[corner, :]
            s0[pl.ds(at + cols, HALO), :] = -corner_e[corner, :]

    lane = lax.broadcasted_iota(jnp.int32, (GROUP, LANES), 1)
    sub = lax.broadcasted_iota(jnp.int32, (GROUP, LANES), 0)

    def add_tap(k, carry):
        code = tap_code[k]
        node = code // LANES
        base = pl.multiple_of(node // GROUP * GROUP, GROUP)
        hit = (lane == lax.rem(code, LANES)) & (sub == node - base)
        s0[pl.ds(base, GROUP), :] += jnp.where(hit, tap_amps[k], 0.0)
        return carry

    lax.fori_loop(0, tap_count[0], add_tap, 0)

    def smooth_and_restrict(source, pre, coef, shunt, pair, rings, store):
        width = pair.shape[1]
        held = []

        def row_of(ref, row):
            return ref[pl.ds(pl.multiple_of(row * width, GROUP), width), :]

        def middle(row, value):
            pre[pl.ds(pl.multiple_of(row * width, GROUP), width), :] = value

        def finish(g, r, row, here, total, weight):
            if r % 2 == 0:
                held.append(total)
            else:
                pair[r // 2] = held.pop() + total
                store(g * (GROUP // 2) + r // 2, r // 2)

        groups = source.shape[0] // width // GROUP
        wave(
            (0, groups), groups - 1, width, coef, 0, shunt, rings,
            lambda r, row, weight: weight * row_of(source, row),
            lambda row: row_of(source, row), middle, finish,
        )

    half = pair1.shape[1]
    start = PAD - (HALO - 2)

    def store1(k, m):
        s1[pl.ds(pl.multiple_of(k * half, GROUP), half), :] = (
            pair[m, pl.ds(start, half, stride=2), :] + pair[m, pl.ds(start + 1, half, stride=2), :]
        )

    smooth_and_restrict(s0, p0, coef0, shunts[0], pair, rings0, store1)
    quarter = cols // 4

    def store2(k, m):
        s2[pl.ds(pl.multiple_of(k * quarter, quarter), quarter), :] = (
            pair1[m, pl.ds(4, quarter, stride=2), :] + pair1[m, pl.ds(5, quarter, stride=2), :]
        )

    smooth_and_restrict(s1, p1, coef1, shunts[1], pair1, rings1, store2)
    rows2 = rows // 4
    per = LANES // rows2
    groups = quarter // per
    for jp in range(groups):
        parts = [
            s2[pl.ds(ROW_PAD // 4 * quarter + jl * groups + jp, rows2, stride=quarter), :]
            for jl in range(per)
        ]
        turned = jnp.concatenate(parts, axis=0).T
        for p in range(pc):
            slab[pl.ds(jp * pc + p, nd, stride=groups * pc), :] = turned[p * nd : (p + 1) * nd]


def up_kernel(dims, shunts, back, s0, p0, s1, p1, coef0, coef1, out, x2, c1, twice1, twice0, *rings):
    rows, cols, nd, pc = dims
    wide = cols + 2 * PAD
    quarter = cols // 4
    wide2 = quarter + 4
    width1 = 2 * wide2
    width0 = 2 * width1
    rows2 = rows // 4 + 4
    pitch2 = x2.shape[0] // rows2
    rings0, rings1 = rings[:9], rings[9:]
    for jw in range(wide2):
        parts = [back[pl.ds(jw * pc + p, nd, stride=wide2 * pc), :] for p in range(pc)]
        turned = jnp.concatenate(parts, axis=0).T
        x2[pl.ds(jw, rows2, stride=pitch2), :] = turned[:rows2]

    def lifted(twice, slot, x):
        count = x.shape[0]
        twice[slot, pl.ds(0, count, stride=2), :] = x
        twice[slot, pl.ds(1, count, stride=2), :] = x
        return twice[slot]

    def fill1(r, row, weight):
        k = jnp.clip(row // 2 - 2, 0, rows2 - 1)
        x = x2[pl.ds(pl.multiple_of(k * pitch2, GROUP), pitch2), :][:wide2]
        return p1[pl.ds(pl.multiple_of(row * width1, GROUP), width1), :] + lifted(
            twice1, r, x
        )

    def source1(row):
        return s1[pl.ds(pl.multiple_of(row * width1, GROUP), width1), :]

    def finish1(g, r, row, here, total, weight):
        c1[pl.ds(pl.multiple_of(row * width1, GROUP), width1), :] = here + weight() * total

    groups1 = s1.shape[0] // width1 // GROUP
    wave(
        (0, groups1), groups1, width1, coef1, 0, shunts[1], rings1,
        fill1, source1, lambda row, value: None, finish1,
    )

    start = PAD - (HALO - 2)

    def fill0(r, row, weight):
        x = c1[pl.ds(pl.multiple_of(row // 2 * width1, GROUP), width1), :]
        return p0[pl.ds(row * wide + start, width0), :] + lifted(twice0, r, x)

    def source0(row):
        return s0[pl.ds(row * wide + start, width0), :]

    first, last = ROW_PAD // GROUP, (ROW_PAD + rows) // GROUP

    def finish0(g, r, row, here, total, weight):
        done = here + weight() * total
        row = jnp.clip(row - ROW_PAD, r, rows - GROUP + r)
        out[row] = done[HALO - 2 : HALO - 2 + cols]

    wave(
        (first - 1, last + 1), last, width0, coef0, start, shunts[0], rings0,
        fill0, source0, lambda row, value: None, finish0,
    )


VMEM = pl.BlockSpec(memory_space=pltpu.VMEM)
SMEM = pl.BlockSpec(memory_space=pltpu.SMEM)
HBM = pl.BlockSpec(memory_space=pltpu.HBM)
PARAMS = pltpu.CompilerParams(vmem_limit_bytes=40 * 2**20)


SMALL = pltpu.CompilerParams(vmem_limit_bytes=16 * 2**20)


def shape(*dims):
    return jax.ShapeDtypeStruct(dims, jnp.float32)


def vmem(*dims):
    return pltpu.VMEM(dims, jnp.float32)


def lane_chunks(x):
    return [x[:, i : i + LANES] for i in range(0, x.shape[1], LANES)]


def block_column(x, k):
    size = x.shape[0]
    lane = lax.broadcasted_iota(jnp.int32, (size, LANES), 1)
    at = lane // size * size + k
    take = functools.partial(jnp.take_along_axis, axis=1, mode="promise_in_bounds")
    return jnp.concatenate([take(c, at) for c in lane_chunks(x)], axis=1)


def block_rows(held, x):
    held[...] = x

    def row(k):
        return jnp.broadcast_to(held[pl.ds(k, 1), :], x.shape)

    return row


def over(size, step, start):
    return lax.fori_loop(0, size, step, start, unroll=size <= GROUP)


def block_product(held, x, *others):
    rows = [block_rows(h, y) for h, y in zip(held, others)]

    def step(k, totals):
        column = block_column(x, k)
        return tuple(t + column * row(k) for t, row in zip(totals, rows))

    return over(x.shape[0], step, tuple(jnp.zeros_like(x) for _ in others))


def block_inverse(held, x):
    size, count = x.shape
    inner = lax.broadcasted_iota(jnp.int32, x.shape, 1) % size
    row_id = lax.broadcasted_iota(jnp.int32, x.shape, 0)

    def step(k, x):
        row = block_rows(held[0], x)(k)
        column = block_column(x, k)
        pivot = block_rows(held[1], column)(k)
        scaled = jnp.where(inner == k, 1.0, row) / pivot
        rest = jnp.where(inner == k, 0.0, x) - column * scaled
        return jnp.where(row_id == k, scaled, rest)

    return over(size, step, x)


def ahead(x, blocks):
    lanes = x.shape[1]
    return pltpu.roll(x, (-blocks * x.shape[0]) % lanes, 1)


def exact_dot(x, y):
    return jnp.dot(x, y, precision=HIGH, preferred_element_type=jnp.float32)


def iota2(rows, cols):
    return (
        lax.broadcasted_iota(jnp.int32, (rows, cols), 0),
        lax.broadcasted_iota(jnp.int32, (rows, cols), 1),
    )


def lanes_for(count):
    return -(-count // LANES) * LANES


def halve_lanes(x, odd=False):
    count = x.shape[1]
    fine, coarse = iota2(count, lanes_for(count // 2))
    hit = fine == 2 * coarse + 1 if odd else fine // 2 == coarse
    return exact_dot(x, hit.astype(jnp.float32))


def double_lanes(x, count):
    coarse, fine = iota2(x.shape[1], count)
    return exact_dot(x, (fine // 2 == coarse).astype(jnp.float32))


def row_pairs(held, x):
    rows = x.shape[0]
    for t, piece in enumerate(lane_chunks(x)):
        held[t, pl.ds(0, rows), :] = piece
    return [
        jnp.concatenate(
            [held[t, pl.ds(k, rows // 2, stride=2), :] for t in range(x.shape[1] // LANES)], axis=1
        )
        for k in range(2)
    ]


def double_rows(held, x):
    rows = x.shape[0]
    for t, piece in enumerate(lane_chunks(x)):
        for k in range(2):
            held[t, pl.ds(k, rows, stride=2), :] = piece
    return jnp.concatenate(
        [held[t, pl.ds(0, 2 * rows), :] for t in range(x.shape[1] // LANES)], axis=1
    )


def place_blocks(dims, from_ref, pitch, to_ref, sets):
    ng, nd_axis, q_rows, q_cols = dims
    per = LANES // q_rows
    group = q_cols // per
    for g in range(ng):
        for d in range(nd_axis):
            for first, stride, base in sets:
                at = (g * nd_axis + d) * pitch + first
                piece = from_ref[pl.ds(at, group, stride=stride), :]
                for jl in range(per):
                    to_ref[
                        pl.ds(base + d * q_cols + jl * group, group), pl.ds(g * q_rows, q_rows)
                    ] = piece[:, jl * q_rows : (jl + 1) * q_rows]


def factor_kernel(dims, pc, gathered, *refs):
    levels = LEVELS - 2
    coefs, (parts, last), (grid, spare, *held) = refs[:levels], refs[levels:levels + 2], refs[levels + 2:]
    ng, nd_axis, q_rows, q_cols = dims
    nj, ni = nd_axis * q_cols, ng * q_rows
    group = q_cols * q_rows // LANES
    place_blocks(dims, gathered, 2 * group, grid, [(0, 1, 0), (group, 1, nj)])
    east, north = grid[pl.ds(0, nj), :], grid[pl.ds(nj, nj), :]
    for k in range(LEVELS - 1):
        shunt = SHUNT_CONDUCT * 4.0 ** (k + 2)
        west, south = pltpu.roll(east, 1, 1), pltpu.roll(north, 1, 0)
        diag = shunt + east + west + north + south
        if k == levels:
            break
        for i, part in enumerate((east, north, RELAXATION / diag)):
            for p in range(pc):
                coefs[k][i, pl.ds(p * nj, nj), :] = part
        even, odd = row_pairs(spare, east)
        east = halve_lanes(even + odd, odd=True)
        even, odd = row_pairs(spare, north)
        north = halve_lanes(odd)
        nj, ni = nj // 2, ni // 2
    size, count = nj, ni * nj
    at, lane = iota2(east.shape[1], count)
    repeat = (lane // size == at).astype(jnp.float32)
    row, col = iota2(size, count)
    col = col % size
    d = jnp.where(col == row, exact_dot(diag, repeat), 0.0)
    d = d - jnp.where(col == row + 1, exact_dot(north, repeat), 0.0)
    d = d - jnp.where(col == row - 1, exact_dot(south, repeat), 0.0)
    c = jnp.where(col == row, -exact_dot(east, repeat), 0.0)
    ct = c
    stride = 1
    level = 0
    while stride * size < count:
        inverse = block_inverse(held, d)
        (r,) = block_product(held, c, ahead(inverse, stride))
        (lx,) = block_product(held, ct, inverse)
        left, lead = ahead(lx, -stride), ahead(lx, stride)
        for i, part in enumerate((r, left, inverse, c, ahead(ct, -stride))):
            parts[level, i] = part
        first, new_c = block_product(held, r, ct, ahead(c, stride))
        (second,) = block_product(held, left, ahead(c, -stride))
        (new_ct,) = block_product(held, lead, ct)
        d = d - first - second
        c, ct = -new_c, -new_ct
        stride *= 2
        level += 1
    last[...] = block_inverse(held, d)


def reduce_and_solve(held, f, parts, last):
    size = f.shape[0]
    block = lax.broadcasted_iota(jnp.int32, f.shape, 1) // size
    levels = parts.shape[0]
    for level in range(levels):
        s = 2**level
        (a,) = block_product(held, parts[level, 0], ahead(f, s))
        (b,) = block_product(held, parts[level, 1], ahead(f, -s))
        f = jnp.where(block % (2 * s) == 0, f - a - b, f)
    (x,) = block_product(held, last[...], f)
    for level in reversed(range(levels)):
        s = 2**level
        (a,) = block_product(held, parts[level, 3], ahead(x, s))
        (b,) = block_product(held, parts[level, 4], ahead(x, -s))
        (new,) = block_product(held, parts[level, 2], f - a - b)
        x = jnp.where(block % (2 * s) == s, new, x)
    return x


def grid_residual(v, source, coef, shunt):
    lanes, rows = v.shape[1], v.shape[0]
    east = coef[0] * (pltpu.roll(v, lanes - 1, 1) - v)
    north = coef[1] * (pltpu.roll(v, rows - 1, 0) - v)
    total = (east - pltpu.roll(east, 1, 1)) + (north - pltpu.roll(north, 1, 0))
    return total + (source - shunt * v)


def coarse_kernel(dims, pc, got, *refs):
    levels = LEVELS - 2
    coefs, (parts, last, back) = refs[:levels], refs[levels : levels + 3]
    grid, spare, shifted, shifted_odd, *held = refs[levels + 3 :]
    ng, nd_axis, q_rows, q_cols = dims
    nj, ni = nd_axis * q_cols, ng * q_rows
    pitch = got.shape[0] // (ng * nd_axis)
    place_blocks(dims, got, pitch, grid, [(p, pc, p * nj) for p in range(pc)])
    source = grid[...]
    stored = []
    for k in range(levels):
        shunt = SHUNT_CONDUCT * 4.0 ** (k + 2)
        coef = coefs[k]
        start = coef[2] * source
        pre = start + coef[2] * grid_residual(start, source, coef, shunt)
        rest = grid_residual(pre, source, coef, shunt)
        stored.append((pre, source, shunt, coef))
        even, odd = row_pairs(spare, rest)
        source = halve_lanes(even + odd)
    size = source.shape[0] // pc
    blocks = ni // 2**levels
    at, lane = iota2(source.shape[1], size * blocks)
    f = None
    picks = [(lane == at * size + p).astype(jnp.float32) for p in range(pc)]
    for p, pick in enumerate(picks):
        part = exact_dot(source[p * size : (p + 1) * size], pick)
        f = part if f is None else f + part
    x = reduce_and_solve(held, f, parts, last)
    fix = jnp.concatenate([exact_dot(x, pick.T) for pick in picks], axis=0)
    for pre, source, shunt, coef in reversed(stored):
        lanes = pre.shape[1]
        v = pre + double_rows(spare, double_lanes(fix, lanes))
        for _ in range(2):
            v = v + coef[2] * grid_residual(v, source, coef, shunt)
        fix = v
    shifted[...] = jnp.zeros_like(shifted)
    rows_p = shifted.shape[0] // pc
    wide = jnp.concatenate([fix, jnp.zeros((fix.shape[0], LANES), jnp.float32)], axis=1)
    wide = pltpu.roll(wide, 2, 1)
    for p in range(pc):
        shifted[pl.ds(p * rows_p + 2, nj), :] = wide[p * nj : (p + 1) * nj]
    lanes = shifted.shape[1]
    shifted_odd[...] = pltpu.roll(shifted[...], lanes - LANES // 2, 1)
    window = q_cols + 4
    for g in range(ng):
        lane_at = g * q_rows
        ref = shifted if lane_at % LANES == 0 else shifted_odd
        lane_at = lane_at // LANES * LANES
        for d in range(nd_axis):
            for p in range(pc):
                piece = ref[pl.ds(p * rows_p + d * q_cols, window), pl.ds(lane_at, LANES)]
                at = (g * nd_axis + d) * window * pc + p
                back[pl.ds(at, window, stride=pc), :] = piece


def coarse_factor(dims, pc, gathered):
    ng, nd_axis, q_rows, q_cols = dims
    nj, ni = nd_axis * q_cols, ng * q_rows
    coefs = []
    for k in range(LEVELS - 2):
        coefs.append(shape(3, pc * nj >> k, lanes_for(ni >> k)))
    size, blocks = nj >> (LEVELS - 2), ni >> (LEVELS - 2)
    flat = (size, blocks * size)
    out = pl.pallas_call(
        functools.partial(factor_kernel, dims, pc),
        out_shape=coefs + [shape(blocks.bit_length() - 1, 5, *flat), shape(*flat)],
        in_specs=[VMEM],
        out_specs=[VMEM] * (len(coefs) + 2),
        scratch_shapes=[vmem(2 * nj, ni), vmem(ni // LANES, nj, LANES)] + [vmem(*flat)] * 2,
        compiler_params=SMALL,
        name="coarse_factor",
    )(gathered)
    return out


def coarse_levels(dims, pc, got, factor):
    ng, nd_axis, q_rows, q_cols = dims
    nj, ni = nd_axis * q_cols, ng * q_rows
    flat = factor[-1].shape
    padded = (pc * (nj + GROUP), ni + LANES)
    return pl.pallas_call(
        functools.partial(coarse_kernel, dims, pc),
        out_shape=shape(ng * nd_axis * (q_cols + 4) * pc, LANES),
        in_specs=[VMEM] * (len(factor) + 1),
        out_specs=VMEM,
        scratch_shapes=[
            vmem(pc * nj, ni), vmem(ni // LANES, pc * nj, LANES), vmem(*padded), vmem(*padded)
        ]
        + [vmem(*flat)] * 2,
        compiler_params=SMALL,
        name="coarse_levels",
    )(got, *factor)


def body(load, east_class, north_class, cond_table, taps, tap_current):
    rows, cols, cands = load.shape
    ng, nd_axis = lax.axis_size("grp"), lax.axis_size("dev")
    nd = ng * nd_axis
    pc = cands // nd
    row_start = lax.axis_index("grp") * rows
    col_start = lax.axis_index("dev") * cols
    all_rows, all_cols = ng * rows, nd_axis * cols
    edge = HALO + 1
    dims = (rows, cols, nd, pc)

    q_rows, q_cols = rows // 4, cols // 4
    coarse_dims = (ng, nd_axis, q_rows, q_cols)
    place = jnp.stack(
        [all_rows - 1 - row_start, all_cols - 1 - col_start, row_start, col_start]
    ).astype(jnp.int32)
    dev_rows = rows * HALO + 2 * edge * rows // LANES
    grp_rows = cols * HALO + 2 * cols
    corner_rows = 2 * HALO * HALO + 8 * GROUP
    share = 2 * q_rows * q_cols // LANES

    strip_e, strip_w, strip_n, strip_s, cond, shares = pl.pallas_call(
        functools.partial(strip_kernel, dims),
        out_shape=[shape(dev_rows, LANES)] * 2
        + [shape(grp_rows, LANES)] * 2
        + [shape(2, cols, rows), shape(nd * share, LANES)],
        in_specs=[SMEM] * 2 + [VMEM] * 3,
        out_specs=[VMEM] * 6,
        scratch_shapes=[vmem(rows // LANES, cols, LANES)],
        compiler_params=PARAMS,
        name="strips",
    )(place, cond_table, load, east_class, north_class)
    from_w, from_e = exchange(strip_e, strip_w, "dev")
    from_n, from_s = exchange(strip_n, strip_s, "grp")
    tap_count, tap_code, tap_amps = pl.pallas_call(
        functools.partial(tap_kernel, dims, all_cols),
        out_shape=[
            jax.ShapeDtypeStruct((1,), jnp.int32),
            jax.ShapeDtypeStruct((taps.shape[1], LANES), jnp.int32),
            shape(taps.shape[1], LANES),
        ],
        in_specs=[SMEM] + [VMEM] * 2,
        out_specs=[SMEM, VMEM, VMEM],
        compiler_params=SMALL,
        name="taps",
    )(place, taps, tap_current)
    corner_e_out, corner_w_out = pl.pallas_call(
        functools.partial(corner_kernel, cols),
        out_shape=[shape(corner_rows, LANES)] * 2,
        in_specs=[VMEM] * 2,
        out_specs=[VMEM] * 2,
        compiler_params=SMALL,
        name="corners",
    )(from_n, from_s)
    shares, corner_e_out, corner_w_out = lax.optimization_barrier(
        (shares, corner_e_out, corner_w_out)
    )
    corner_w, corner_e = exchange(corner_e_out, corner_w_out, "dev")
    gathered = lax.all_to_all(
        shares.reshape(nd, share, LANES), AXES, split_axis=0, concat_axis=0, tiled=True
    )
    factor = coarse_factor(coarse_dims, pc, gathered.reshape(-1, LANES))

    wide0 = cols + 2 * PAD
    ext_rows = rows + 2 * ROW_PAD
    wide1 = cols // 2 + HALO - 2
    rows1 = rows // 2 + ROW_PAD
    lanes0 = lanes_for(ext_rows)
    coef0, coef1 = pl.pallas_call(
        functools.partial(coef_kernel, dims),
        out_shape=[
            shape(3, lanes0 // LANES, wide0, LANES),
            shape(3, lanes_for(lanes0 // 2) // LANES, wide1, LANES),
        ],
        in_specs=[VMEM] * 7,
        out_specs=[VMEM] * 2,
        scratch_shapes=[vmem(wide0, lanes0), vmem(lanes0 // LANES, wide0, LANES)],
        compiler_params=SMALL,
        name="coefs",
    )(cond, from_w, from_e, from_n, from_s, corner_w, corner_e)

    s2_rows = rows1 // 2 * q_cols
    slab_rows = pc * q_rows * q_cols // LANES
    shunts = (SHUNT_CONDUCT, SHUNT_CONDUCT * 4.0)
    s0, p0, s1, p1, slab = pl.pallas_call(
        functools.partial(down_kernel, dims, shunts),
        out_shape=[
            shape(ext_rows * wide0, LANES),
            shape(ext_rows * wide0, LANES),
            shape(rows1 * wide1, LANES),
            shape(rows1 * wide1, LANES),
            shape(nd * slab_rows, LANES),
        ],
        in_specs=[SMEM] * 3 + [HBM] * 3 + [VMEM] * 6,
        out_specs=[VMEM] * 5,
        scratch_shapes=[
            vmem(rows, cols, LANES),
            vmem(rows * HALO, LANES),
            vmem(rows * HALO, LANES),
            pltpu.SemaphoreType.DMA((3,)),
            vmem(s2_rows, LANES),
            vmem(GROUP // 2, wide0, LANES),
            vmem(GROUP // 2, wide1, LANES),
        ]
        + rings_for(wide0)
        + rings_for(wide1),
        compiler_params=PARAMS,
        name="fine_down",
    )(tap_count, tap_code.reshape(-1), tap_amps.reshape(-1), load, from_w, from_e, from_n, from_s, corner_w, corner_e, coef0, coef1)

    got = lax.all_to_all(
        slab.reshape(nd, slab_rows, LANES), AXES, split_axis=0, concat_axis=0, tiled=True
    )
    back = coarse_levels(coarse_dims, pc, got.reshape(-1, LANES), factor)
    back = back.reshape(nd, (q_cols + 4) * pc, LANES)
    back = lax.all_to_all(back, AXES, split_axis=0, concat_axis=0, tiled=True)
    pitch2 = -(-(q_cols + 4) // GROUP) * GROUP
    return pl.pallas_call(
        functools.partial(up_kernel, dims, shunts),
        out_shape=shape(rows, cols, LANES),
        in_specs=[VMEM] * 7,
        out_specs=VMEM,
        scratch_shapes=[
            vmem((q_rows + 4) * pitch2, LANES),
            vmem(rows1 * wide1, LANES),
            vmem(GROUP, wide1, LANES),
            vmem(GROUP, 2 * wide1, LANES),
        ]
        + rings_for(2 * wide1)
        + rings_for(wide1),
        compiler_params=PARAMS,
        name="fine_up",
    )(back.reshape(-1, LANES), s0, p0, s1, p1, coef0, coef1)


def solution(mesh):
    return jax.shard_map(
        body,
        mesh=mesh,
        in_specs=(P("grp", "dev", None), P("grp", "dev"), P("grp", "dev"), P(), P(), P()),
        out_specs=P("grp", "dev", None),
        check_vma=False,
    )
```

```python
import functools

import jax
import jax.numpy as jnp
from jax import lax
from jax.experimental import pallas as pl
from jax.experimental.pallas import tpu as pltpu
from jax.sharding import PartitionSpec as P


LEVELS = 5
RELAXATION = 0.8
SHUNT_CONDUCT = 0.01
AXES = ("grp", "dev")
HIGH = lax.Precision.HIGHEST

HALO = 10
PAD = 12
ROW_PAD = 16
LANES = 128
GROUP = 8


def exchange(tail, head, axis):
    count = lax.axis_size(axis)
    up = [(i, i + 1) for i in range(count - 1)]
    down = [(i + 1, i) for i in range(count - 1)]
    return lax.ppermute(tail, axis, up), lax.ppermute(head, axis, down)


RING = 4 * GROUP


def wave(groups, stop, width, coef, coef_first, shunt, rings, fill, source, middle, finish):
    ring_e, ring_n, ring_w, ring_a, ring_b, flux_b, again_b, flux_c, turn = rings
    low, high = groups
    per_tile = LANES // GROUP
    for ref in rings:
        ref[...] = jnp.zeros_like(ref)

    def at(ref, row, ahead=0):
        base = pl.multiple_of(lax.rem(row, RING) * width, GROUP)
        return ref[pl.ds(base + ahead, width), :]

    def put(ref, row, value):
        base = pl.multiple_of(lax.rem(row, RING) * width, GROUP)
        ref[pl.ds(base, width), :] = value

    def balance(ring, row, before, slot):
        here = at(ring, row)
        east = at(ring_e, row) * (at(ring, row + 1) - here)
        north = at(ring_n, row) * (at(ring, row, 1) - here)
        turn[slot, pl.ds(GROUP, width), :] = north
        south = turn[slot, pl.ds(GROUP - 1, width), :]
        total = (east - before) + (north - south) + (source(row) - shunt * here)
        return here, east, total

    def go(t, carry):
        g = jnp.minimum(t, high - 1)
        shift = lax.rem(LANES - lax.rem(g, per_tile) * GROUP, LANES)
        found = [
            pltpu.roll(coef[k, g // per_tile, pl.ds(coef_first, width), :], shift, 1)
            for k in range(3)
        ]
        for r in range(GROUP):
            row = g * GROUP + r
            east, north, weight = (
                jnp.broadcast_to(x[:, r : r + 1], (width, LANES)) for x in found
            )
            put(ring_e, row, east)
            put(ring_n, row, north)
            put(ring_w, row, weight)
            put(ring_a, row, fill(r, row, weight))
        g = jnp.clip(t - 1, low, high - 1)
        flux = jnp.where(t > high, again_b[...], flux_b[...])
        again_b[...] = flux
        for r in range(GROUP):
            row = g * GROUP + r
            here, flux, total = balance(ring_a, row, flux, r)
            value = here + at(ring_w, row) * total
            put(ring_b, row, value)
            middle(row, value)
        flux_b[...] = flux
        g = jnp.clip(t - 2, low, high - 1)
        flux = flux_c[...]
        for r in range(GROUP):
            row = g * GROUP + r
            here, flux, total = balance(ring_b, row, flux, GROUP + r)
            finish(g, r, row, here, total, lambda row=row: at(ring_w, row))
        flux_c[...] = flux
        return carry

    lax.fori_loop(low, stop + 2, go, 0)


def rings_for(width):
    ring = vmem(RING * width + GROUP, LANES)
    return [ring] * 5 + [vmem(width, LANES)] * 3 + [vmem(2 * GROUP, width + GROUP, LANES)]


def strip_kernel(
    dims, place, table, load, east_class, north_class,
    strip_e, strip_w, strip_n, strip_s, cond, shares, held,
):
    rows, cols, nd, _ = dims
    edge = HALO + 1

    def copy(i, carry):
        strip_e[pl.ds(i * HALO, HALO), :] = load[i, cols - HALO :, :]
        strip_w[pl.ds(i * HALO, HALO), :] = load[i, :HALO, :]
        return carry

    lax.fori_loop(0, rows, copy, 0, unroll=8)
    for i in range(HALO):
        strip_n[pl.ds(i * cols, cols), :] = load[rows - HALO + i]
        strip_s[pl.ds(i * cols, cols), :] = load[i]
    coarse = []
    for k, classes in enumerate((east_class, north_class)):
        kind = classes[...]
        value = jnp.zeros(kind.shape, jnp.float32)
        for c in range(table.shape[0]):
            value = jnp.where(kind == c, table[c], value)
        node = lax.broadcasted_iota(jnp.int32, kind.shape, 1 - k)
        turned = jnp.where(node == place[k], 0.0, value)
        cond[k] = turned
        pieces = rows // LANES
        for h in range(pieces):
            at = pl.ds(rows * HALO + k * edge * pieces + h, edge, stride=pieces)
            part = turned[:, h * LANES : (h + 1) * LANES]
            strip_e[at, :] = part[cols - edge :]
            strip_w[at, :] = part[:edge]
        at = pl.ds(cols * HALO + k * cols, cols)
        strip_n[at, :] = pltpu.roll(turned, edge, 1)[:, :LANES]
        strip_s[at, :] = turned[:, :LANES]
        for _ in range(2):
            even, odd = row_pairs(held, turned)
            turned = halve_lanes(even + odd, odd=True) if k == 0 else halve_lanes(odd)
        coarse.append(turned)
    q_rows, q_cols = rows // 4, cols // 4
    per = LANES // q_rows
    group = q_cols // per
    for k, value in enumerate(coarse):
        for jl in range(per):
            shares[pl.ds(k * group, group), pl.ds(jl * q_rows, q_rows)] = value[
                jl * group : (jl + 1) * group, :q_rows
            ]
    mine = shares[pl.ds(0, 2 * group), :]
    for q in range(1, nd):
        shares[pl.ds(q * 2 * group, 2 * group), :] = mine


def corner_kernel(cols, north, south, out_e, out_w):
    edge = HALO + 1
    cond_at = 2 * HALO * HALO
    for ref in (out_e, out_w):
        ref[...] = jnp.zeros_like(ref)
    for end, strip in enumerate((north, south)):
        for i in range(HALO):
            at = pl.ds((end * HALO + i) * HALO, HALO)
            out_e[at, :] = strip[pl.ds((i + 1) * cols - HALO, HALO), :]
            out_w[at, :] = strip[pl.ds(i * cols, HALO), :]
        for k in range(2):
            at = pl.ds(cond_at + (end * 2 + k) * 2 * GROUP, edge)
            first = cols * HALO + k * cols
            out_e[at, :] = strip[pl.ds(first + cols - edge, edge), :]
            out_w[at, :] = strip[pl.ds(first, edge), :]


def coef_kernel(
    dims, cond, west, east, north, south, corner_w, corner_e, coef0, coef1, grid, held
):
    rows, cols, _, _ = dims
    edge = HALO + 1
    wide1 = coef1.shape[2]
    pieces = rows // LANES
    first = ROW_PAD - edge
    grids = []
    for k in range(2):
        grid[...] = jnp.zeros_like(grid)
        grid[pl.ds(PAD, cols), pl.ds(ROW_PAD, rows)] = cond[k]
        for strip, col in ((west, PAD - edge), (east, PAD + cols)):
            for h in range(pieces):
                at = pl.ds(rows * HALO + k * edge * pieces + h, edge, stride=pieces)
                grid[pl.ds(col, edge), pl.ds(ROW_PAD + h * LANES, LANES)] = strip[at, :]
        for end, (strip, row) in enumerate(((north, first), (south, ROW_PAD + rows))):
            at = pl.ds(cols * HALO + k * cols, cols)
            grid[pl.ds(PAD, cols), pl.ds(row, edge)] = strip[at, :][:, :edge]
            at = pl.ds(2 * HALO * HALO + (end * 2 + k) * 2 * GROUP, edge)
            for corner, col in ((corner_w, PAD - edge), (corner_e, PAD + cols)):
                grid[pl.ds(col, edge), pl.ds(row, edge)] = corner[at, :][:, :edge]
        grids.append(grid[...])

    def put(coef, east, west, north, south, shunt):
        weight = RELAXATION / (shunt + east + west + north + south)
        for i, value in enumerate((east, north, weight)):
            for t, piece in enumerate(lane_chunks(value)):
                coef[i, t] = piece

    east, north = grids
    put(coef0, east, pltpu.roll(east, 1, 1), north, pltpu.roll(north, 1, 0), SHUNT_CONDUCT)
    tiles = east.shape[1] // LANES

    def picked(start):
        at = pl.ds(start, wide1, stride=2)
        return jnp.concatenate([held[t, at, :] for t in range(tiles)], axis=1)

    start = PAD - (HALO - 2)
    for t, piece in enumerate(lane_chunks(east)):
        held[t] = piece
    east = halve_lanes(picked(start) + picked(start + 1), odd=True)
    for t, piece in enumerate(lane_chunks(north)):
        held[t] = piece
    north, south = halve_lanes(picked(start + 1)), halve_lanes(picked(start - 1))
    put(coef1, east, pltpu.roll(east, 1, 1), north, south, 4.0 * SHUNT_CONDUCT)


def tap_kernel(dims, all_cols, place, taps, currents, count, codes, amps):
    rows, cols, _, _ = dims
    node, current = taps[...], currents[...]
    lead = node.shape[0]
    row_at = node // all_cols
    i = row_at - place[2]
    j = node - row_at * all_cols - place[3]
    inside = (i >= -HALO) & (i < rows + HALO) & (j >= -HALO) & (j < cols + HALO)
    lane = lax.broadcasted_iota(jnp.int32, node.shape, 1)
    code = ((i + ROW_PAD) * (cols + 2 * PAD) + j + PAD) * LANES + lane
    flags = jnp.where(inside, 1.0, 0.0)
    at, to = iota2(LANES, LANES)
    upto = exact_dot(flags, (at <= to).astype(jnp.float32))
    at, to = iota2(lead, lead)
    before = exact_dot((at > to).astype(jnp.float32), upto)[:, LANES - 1 :]
    slot = jnp.where(inside, (upto + before).astype(jnp.int32) - 1, -1)
    total = jnp.sum(flags).astype(jnp.int32)
    count[0] = total
    codes[...] = jnp.zeros_like(codes)
    amps[...] = jnp.zeros_like(amps)
    wanted = lax.broadcasted_iota(jnp.int32, (LANES, LANES), 0)
    code = code.astype(jnp.float32)

    def fill(chunk, carry):
        found = jnp.zeros((LANES, LANES), jnp.float32)
        amount = jnp.zeros((LANES, LANES), jnp.float32)
        for k in range(lead):
            hit = wanted + chunk * LANES == jnp.broadcast_to(slot[k : k + 1], wanted.shape)
            found += jnp.where(hit, jnp.broadcast_to(code[k : k + 1], wanted.shape), 0.0)
            amount += jnp.where(hit, jnp.broadcast_to(current[k : k + 1], wanted.shape), 0.0)
        codes[pl.ds(chunk, 1), :] = jnp.sum(found.T, axis=0, keepdims=True).astype(jnp.int32)
        amps[pl.ds(chunk, 1), :] = jnp.sum(amount.T, axis=0, keepdims=True)
        return carry

    lax.fori_loop(0, (total + LANES - 1) // LANES, fill, 0)


def down_kernel(
    dims, shunts, tap_count, tap_code, tap_amps, own_hbm, west_hbm, east_hbm, north, south,
    corner_w, corner_e, coef0, coef1, s0_out, p0_out, s1, p1, slab, s0, p0, own, west, east, sems,
    s2, pair, pair1, *rings,
):
    rows, cols, nd, pc = dims
    wide = cols + 2 * PAD
    rings0, rings1 = rings[:9], rings[9:]

    moves = [
        pltpu.make_async_copy(source.at[pl.ds(0, here.shape[0])], here, sems.at[k])
        for k, (source, here) in enumerate(((own_hbm, own), (west_hbm, west), (east_hbm, east)))
    ]
    for move in moves:
        move.start()
    s0[...] = jnp.zeros_like(s0)
    for move in moves:
        move.wait()
    first = ROW_PAD - HALO

    def copy_own(i, carry):
        base = (i + ROW_PAD) * wide
        s0[pl.ds(base + PAD, cols), :] = -own[i]
        s0[pl.ds(base + PAD - HALO, HALO), :] = -west[pl.ds(i * HALO, HALO), :]
        s0[pl.ds(base + PAD + cols, HALO), :] = -east[pl.ds(i * HALO, HALO), :]
        return carry

    lax.fori_loop(0, rows, copy_own, 0, unroll=8)
    for k, (strip, base) in enumerate(((north, first), (south, ROW_PAD + rows))):
        for i in range(HALO):
            at = (base + i) * wide + PAD
            corner = pl.ds((k * HALO + i) * HALO, HALO)
            s0[pl.ds(at, cols), :] = -strip[i * cols : (i + 1) * cols, :]
            s0[pl.ds(at - HALO, HALO), :] = -corner_w[corner, :]
            s0[pl.ds(at + cols, HALO), :] = -corner_e[corner, :]

    lane = lax.broadcasted_iota(jnp.int32, (GROUP, LANES), 1)
    sub = lax.broadcasted_iota(jnp.int32, (GROUP, LANES), 0)

    def add_tap(k, carry):
        code = tap_code[k]
        node = code // LANES
        base = pl.multiple_of(node // GROUP * GROUP, GROUP)
        hit = (lane == lax.rem(code, LANES)) & (sub == node - base)
        s0[pl.ds(base, GROUP), :] += jnp.where(hit, tap_amps[k], 0.0)
        return carry

    lax.fori_loop(0, tap_count[0], add_tap, 0)
    save_s0 = pltpu.make_async_copy(s0, s0_out, sems.at[3])
    save_p0 = pltpu.make_async_copy(p0, p0_out, sems.at[4])
    save_s0.start()

    def smooth_and_restrict(source, pre, coef, shunt, pair, rings, store):
        width = pair.shape[1]
        held = []

        def row_of(ref, row):
            return ref[pl.ds(pl.multiple_of(row * width, GROUP), width), :]

        def middle(row, value):
            pre[pl.ds(pl.multiple_of(row * width, GROUP), width), :] = value

        def finish(g, r, row, here, total, weight):
            if r % 2 == 0:
                held.append(total)
            else:
                pair[r // 2] = held.pop() + total
                store(g * (GROUP // 2) + r // 2, r // 2)

        groups = source.shape[0] // width // GROUP
        wave(
            (0, groups), groups - 1, width, coef, 0, shunt, rings,
            lambda r, row, weight: weight * row_of(source, row),
            lambda row: row_of(source, row), middle, finish,
        )

    half = pair1.shape[1]
    start = PAD - (HALO - 2)

    def store1(k, m):
        s1[pl.ds(pl.multiple_of(k * half, GROUP), half), :] = (
            pair[m, pl.ds(start, half, stride=2), :] + pair[m, pl.ds(start + 1, half, stride=2), :]
        )

    smooth_and_restrict(s0, p0, coef0, shunts[0], pair, rings0, store1)
    save_p0.start()
    quarter = cols // 4

    def store2(k, m):
        s2[pl.ds(pl.multiple_of(k * quarter, quarter), quarter), :] = (
            pair1[m, pl.ds(4, quarter, stride=2), :] + pair1[m, pl.ds(5, quarter, stride=2), :]
        )

    smooth_and_restrict(s1, p1, coef1, shunts[1], pair1, rings1, store2)
    rows2 = rows // 4
    per = LANES // rows2
    groups = quarter // per
    for jp in range(groups):
        parts = [
            s2[pl.ds(ROW_PAD // 4 * quarter + jl * groups + jp, rows2, stride=quarter), :]
            for jl in range(per)
        ]
        turned = jnp.concatenate(parts, axis=0).T
        for p in range(pc):
            slab[pl.ds(jp * pc + p, nd, stride=groups * pc), :] = turned[p * nd : (p + 1) * nd]
    save_s0.wait()
    save_p0.wait()


def up_kernel(
    dims, shunts, back, s0_hbm, p0_hbm, s1, p1, coef0, coef1, out, s0, p0, sems, x2, c1, twice1,
    twice0, *rings,
):
    rows, cols, nd, pc = dims
    wide = cols + 2 * PAD
    quarter = cols // 4
    wide2 = quarter + 4
    width1 = 2 * wide2
    width0 = 2 * width1
    rows2 = rows // 4 + 4
    pitch2 = x2.shape[0] // rows2
    rings0, rings1 = rings[:9], rings[9:]
    moves = [
        pltpu.make_async_copy(far, near, sems.at[k])
        for k, (far, near) in enumerate(((s0_hbm, s0), (p0_hbm, p0)))
    ]
    for move in moves:
        move.start()
    for jw in range(wide2):
        parts = [back[pl.ds(jw * pc + p, nd, stride=wide2 * pc), :] for p in range(pc)]
        turned = jnp.concatenate(parts, axis=0).T
        x2[pl.ds(jw, rows2, stride=pitch2), :] = turned[:rows2]

    def lifted(twice, slot, x):
        count = x.shape[0]
        twice[slot, pl.ds(0, count, stride=2), :] = x
        twice[slot, pl.ds(1, count, stride=2), :] = x
        return twice[slot]

    def fill1(r, row, weight):
        k = jnp.clip(row // 2 - 2, 0, rows2 - 1)
        x = x2[pl.ds(pl.multiple_of(k * pitch2, GROUP), pitch2), :][:wide2]
        return p1[pl.ds(pl.multiple_of(row * width1, GROUP), width1), :] + lifted(
            twice1, r, x
        )

    def source1(row):
        return s1[pl.ds(pl.multiple_of(row * width1, GROUP), width1), :]

    def finish1(g, r, row, here, total, weight):
        c1[pl.ds(pl.multiple_of(row * width1, GROUP), width1), :] = here + weight() * total

    groups1 = s1.shape[0] // width1 // GROUP
    wave(
        (0, groups1), groups1, width1, coef1, 0, shunts[1], rings1,
        fill1, source1, lambda row, value: None, finish1,
    )

    start = PAD - (HALO - 2)

    def fill0(r, row, weight):
        x = c1[pl.ds(pl.multiple_of(row // 2 * width1, GROUP), width1), :]
        return p0[pl.ds(row * wide + start, width0), :] + lifted(twice0, r, x)

    def source0(row):
        return s0[pl.ds(row * wide + start, width0), :]

    first, last = ROW_PAD // GROUP, (ROW_PAD + rows) // GROUP
    for move in moves:
        move.wait()

    def finish0(g, r, row, here, total, weight):
        done = here + weight() * total
        row = jnp.clip(row - ROW_PAD, r, rows - GROUP + r)
        out[row] = done[HALO - 2 : HALO - 2 + cols]

    wave(
        (first - 1, last + 1), last, width0, coef0, start, shunts[0], rings0,
        fill0, source0, lambda row, value: None, finish0,
    )


VMEM = pl.BlockSpec(memory_space=pltpu.VMEM)
SMEM = pl.BlockSpec(memory_space=pltpu.SMEM)
HBM = pl.BlockSpec(memory_space=pltpu.HBM)
PARAMS = pltpu.CompilerParams(vmem_limit_bytes=60 * 1024 * 2**10)


SMALL = pltpu.CompilerParams(vmem_limit_bytes=16 * 2**20)


def shape(*dims):
    return jax.ShapeDtypeStruct(dims, jnp.float32)


def vmem(*dims):
    return pltpu.VMEM(dims, jnp.float32)


def lane_chunks(x):
    return [x[:, i : i + LANES] for i in range(0, x.shape[1], LANES)]


def block_column(x, k):
    size = x.shape[0]
    lane = lax.broadcasted_iota(jnp.int32, (size, LANES), 1)
    at = lane // size * size + k
    take = functools.partial(jnp.take_along_axis, axis=1, mode="promise_in_bounds")
    return jnp.concatenate([take(c, at) for c in lane_chunks(x)], axis=1)


def block_rows(held, x):
    held[...] = x

    def row(k):
        return jnp.broadcast_to(held[pl.ds(k, 1), :], x.shape)

    return row


def over(size, step, start):
    return lax.fori_loop(0, size, step, start, unroll=size <= GROUP)


def block_product(held, x, *others):
    rows = [block_rows(h, y) for h, y in zip(held, others)]

    def step(k, totals):
        column = block_column(x, k)
        return tuple(t + column * row(k) for t, row in zip(totals, rows))

    return over(x.shape[0], step, tuple(jnp.zeros_like(x) for _ in others))


def block_inverse(held, x):
    size, _ = x.shape
    inner = lax.broadcasted_iota(jnp.int32, x.shape, 1) % size
    row_id = lax.broadcasted_iota(jnp.int32, x.shape, 0)

    def step(k, x):
        row = block_rows(held[0], x)(k)
        column = block_column(x, k)
        pivot = block_rows(held[1], column)(k)
        scaled = jnp.where(inner == k, 1.0, row) / pivot
        rest = jnp.where(inner == k, 0.0, x) - column * scaled
        return jnp.where(row_id == k, scaled, rest)

    return over(size, step, x)


def ahead(x, blocks):
    lanes = x.shape[1]
    return pltpu.roll(x, (-blocks * x.shape[0]) % lanes, 1)


def exact_dot(x, y):
    return jnp.dot(x, y, precision=HIGH, preferred_element_type=jnp.float32)


def iota2(rows, cols):
    return (
        lax.broadcasted_iota(jnp.int32, (rows, cols), 0),
        lax.broadcasted_iota(jnp.int32, (rows, cols), 1),
    )


def lanes_for(count):
    return -(-count // LANES) * LANES


def halve_lanes(x, odd=False):
    count = x.shape[1]
    fine, coarse = iota2(count, lanes_for(count // 2))
    hit = fine == 2 * coarse + 1 if odd else fine // 2 == coarse
    return exact_dot(x, hit.astype(jnp.float32))


def double_lanes(x, count):
    coarse, fine = iota2(x.shape[1], count)
    return exact_dot(x, (fine // 2 == coarse).astype(jnp.float32))


def row_pairs(held, x):
    rows = x.shape[0]
    for t, piece in enumerate(lane_chunks(x)):
        held[t, pl.ds(0, rows), :] = piece
    return [
        jnp.concatenate(
            [held[t, pl.ds(k, rows // 2, stride=2), :] for t in range(x.shape[1] // LANES)], axis=1
        )
        for k in range(2)
    ]


def double_rows(held, x):
    rows = x.shape[0]
    for t, piece in enumerate(lane_chunks(x)):
        for k in range(2):
            held[t, pl.ds(k, rows, stride=2), :] = piece
    return jnp.concatenate(
        [held[t, pl.ds(0, 2 * rows), :] for t in range(x.shape[1] // LANES)], axis=1
    )


def place_blocks(dims, from_ref, pitch, to_ref, sets):
    ng, nd_axis, q_rows, q_cols = dims
    per = LANES // q_rows
    group = q_cols // per
    for g in range(ng):
        for d in range(nd_axis):
            for first, stride, base in sets:
                at = (g * nd_axis + d) * pitch + first
                piece = from_ref[pl.ds(at, group, stride=stride), :]
                for jl in range(per):
                    to_ref[
                        pl.ds(base + d * q_cols + jl * group, group), pl.ds(g * q_rows, q_rows)
                    ] = piece[:, jl * q_rows : (jl + 1) * q_rows]


def factor_kernel(dims, pc, gathered, *refs):
    levels = LEVELS - 2
    coefs, (parts, last), (grid, spare, *held) = refs[:levels], refs[levels:levels + 2], refs[levels + 2:]
    ng, nd_axis, q_rows, q_cols = dims
    nj, ni = nd_axis * q_cols, ng * q_rows
    group = q_cols * q_rows // LANES
    place_blocks(dims, gathered, 2 * group, grid, [(0, 1, 0), (group, 1, nj)])
    east, north = grid[pl.ds(0, nj), :], grid[pl.ds(nj, nj), :]
    for k in range(LEVELS - 1):
        shunt = SHUNT_CONDUCT * 4.0 ** (k + 2)
        west, south = pltpu.roll(east, 1, 1), pltpu.roll(north, 1, 0)
        diag = shunt + east + west + north + south
        if k == levels:
            break
        for i, part in enumerate((east, north, RELAXATION / diag)):
            for p in range(pc):
                coefs[k][i, pl.ds(p * nj, nj), :] = part
        even, odd = row_pairs(spare, east)
        east = halve_lanes(even + odd, odd=True)
        even, odd = row_pairs(spare, north)
        north = halve_lanes(odd)
        nj, ni = nj // 2, ni // 2
    size, count = nj, ni * nj
    at, lane = iota2(east.shape[1], count)
    repeat = (lane // size == at).astype(jnp.float32)
    row, col = iota2(size, count)
    col = col % size
    d = jnp.where(col == row, exact_dot(diag, repeat), 0.0)
    d = d - jnp.where(col == row + 1, exact_dot(north, repeat), 0.0)
    d = d - jnp.where(col == row - 1, exact_dot(south, repeat), 0.0)
    c = jnp.where(col == row, -exact_dot(east, repeat), 0.0)
    ct = c
    stride = 1
    level = 0
    while stride * size < count:
        inverse = block_inverse(held, d)
        (r,) = block_product(held, c, ahead(inverse, stride))
        (lx,) = block_product(held, ct, inverse)
        left, lead = ahead(lx, -stride), ahead(lx, stride)
        for i, part in enumerate((r, left, inverse, c, ahead(ct, -stride))):
            parts[level, i] = part
        first, new_c = block_product(held, r, ct, ahead(c, stride))
        (second,) = block_product(held, left, ahead(c, -stride))
        (new_ct,) = block_product(held, lead, ct)
        d = d - first - second
        c, ct = -new_c, -new_ct
        stride *= 2
        level += 1
    last[...] = block_inverse(held, d)


def reduce_and_solve(held, f, parts, last):
    size = f.shape[0]
    block = lax.broadcasted_iota(jnp.int32, f.shape, 1) // size
    levels = parts.shape[0]
    for level in range(levels):
        s = 2**level
        (a,) = block_product(held, parts[level, 0], ahead(f, s))
        (b,) = block_product(held, parts[level, 1], ahead(f, -s))
        f = jnp.where(block % (2 * s) == 0, f - a - b, f)
    (x,) = block_product(held, last[...], f)
    for level in reversed(range(levels)):
        s = 2**level
        (a,) = block_product(held, parts[level, 3], ahead(x, s))
        (b,) = block_product(held, parts[level, 4], ahead(x, -s))
        (new,) = block_product(held, parts[level, 2], f - a - b)
        x = jnp.where(block % (2 * s) == s, new, x)
    return x


def grid_residual(v, source, coef, shunt):
    lanes, rows = v.shape[1], v.shape[0]
    east = coef[0] * (pltpu.roll(v, lanes - 1, 1) - v)
    north = coef[1] * (pltpu.roll(v, rows - 1, 0) - v)
    total = (east - pltpu.roll(east, 1, 1)) + (north - pltpu.roll(north, 1, 0))
    return total + (source - shunt * v)


def coarse_kernel(dims, pc, got, *refs):
    levels = LEVELS - 2
    coefs, (parts, last, back) = refs[:levels], refs[levels : levels + 3]
    grid, spare, shifted, shifted_odd, *held = refs[levels + 3 :]
    ng, nd_axis, q_rows, q_cols = dims
    nj, ni = nd_axis * q_cols, ng * q_rows
    pitch = got.shape[0] // (ng * nd_axis)
    place_blocks(dims, got, pitch, grid, [(p, pc, p * nj) for p in range(pc)])
    source = grid[...]
    stored = []
    for k in range(levels):
        shunt = SHUNT_CONDUCT * 4.0 ** (k + 2)
        coef = coefs[k]
        start = coef[2] * source
        pre = start + coef[2] * grid_residual(start, source, coef, shunt)
        rest = grid_residual(pre, source, coef, shunt)
        stored.append((pre, source, shunt, coef))
        even, odd = row_pairs(spare, rest)
        source = halve_lanes(even + odd)
    size = source.shape[0] // pc
    blocks = ni // 2**levels
    at, lane = iota2(source.shape[1], size * blocks)
    f = None
    picks = [(lane == at * size + p).astype(jnp.float32) for p in range(pc)]
    for p, pick in enumerate(picks):
        part = exact_dot(source[p * size : (p + 1) * size], pick)
        f = part if f is None else f + part
    x = reduce_and_solve(held, f, parts, last)
    fix = jnp.concatenate([exact_dot(x, pick.T) for pick in picks], axis=0)
    for pre, source, shunt, coef in reversed(stored):
        lanes = pre.shape[1]
        v = pre + double_rows(spare, double_lanes(fix, lanes))
        for _ in range(2):
            v = v + coef[2] * grid_residual(v, source, coef, shunt)
        fix = v
    shifted[...] = jnp.zeros_like(shifted)
    rows_p = shifted.shape[0] // pc
    wide = jnp.concatenate([fix, jnp.zeros((fix.shape[0], LANES), jnp.float32)], axis=1)
    wide = pltpu.roll(wide, 2, 1)
    for p in range(pc):
        shifted[pl.ds(p * rows_p + 2, nj), :] = wide[p * nj : (p + 1) * nj]
    lanes = shifted.shape[1]
    shifted_odd[...] = pltpu.roll(shifted[...], lanes - LANES // 2, 1)
    window = q_cols + 4
    for g in range(ng):
        lane_at = g * q_rows
        ref = shifted if lane_at % LANES == 0 else shifted_odd
        lane_at = lane_at // LANES * LANES
        for d in range(nd_axis):
            for p in range(pc):
                piece = ref[pl.ds(p * rows_p + d * q_cols, window), pl.ds(lane_at, LANES)]
                at = (g * nd_axis + d) * window * pc + p
                back[pl.ds(at, window, stride=pc), :] = piece


def coarse_factor(dims, pc, gathered):
    ng, nd_axis, q_rows, q_cols = dims
    nj, ni = nd_axis * q_cols, ng * q_rows
    coefs = []
    for k in range(LEVELS - 2):
        coefs.append(shape(3, pc * nj >> k, lanes_for(ni >> k)))
    size, blocks = nj >> (LEVELS - 2), ni >> (LEVELS - 2)
    flat = (size, blocks * size)
    out = pl.pallas_call(
        functools.partial(factor_kernel, dims, pc),
        out_shape=coefs + [shape(blocks.bit_length() - 1, 5, *flat), shape(*flat)],
        in_specs=[VMEM],
        out_specs=[VMEM] * (len(coefs) + 2),
        scratch_shapes=[vmem(2 * nj, ni), vmem(ni // LANES, nj, LANES)] + [vmem(*flat)] * 2,
        compiler_params=SMALL,
        name="coarse_factor",
    )(gathered)
    return out


def coarse_levels(dims, pc, got, factor):
    ng, nd_axis, q_rows, q_cols = dims
    nj, ni = nd_axis * q_cols, ng * q_rows
    flat = factor[-1].shape
    padded = (pc * (nj + GROUP), ni + LANES)
    return pl.pallas_call(
        functools.partial(coarse_kernel, dims, pc),
        out_shape=shape(ng * nd_axis * (q_cols + 4) * pc, LANES),
        in_specs=[VMEM] * (len(factor) + 1),
        out_specs=VMEM,
        scratch_shapes=[
            vmem(pc * nj, ni), vmem(ni // LANES, pc * nj, LANES), vmem(*padded), vmem(*padded)
        ]
        + [vmem(*flat)] * 2,
        compiler_params=SMALL,
        name="coarse_levels",
    )(got, *factor)


def body(load, east_class, north_class, cond_table, taps, tap_current):
    rows, cols, cands = load.shape
    ng, nd_axis = lax.axis_size("grp"), lax.axis_size("dev")
    nd = ng * nd_axis
    pc = cands // nd
    row_start = lax.axis_index("grp") * rows
    col_start = lax.axis_index("dev") * cols
    all_rows, all_cols = ng * rows, nd_axis * cols
    edge = HALO + 1
    dims = (rows, cols, nd, pc)

    q_rows, q_cols = rows // 4, cols // 4
    coarse_dims = (ng, nd_axis, q_rows, q_cols)
    place = jnp.stack(
        [all_rows - 1 - row_start, all_cols - 1 - col_start, row_start, col_start]
    ).astype(jnp.int32)
    dev_rows = rows * HALO + 2 * edge * rows // LANES
    grp_rows = cols * HALO + 2 * cols
    corner_rows = 2 * HALO * HALO + 8 * GROUP
    share = 2 * q_rows * q_cols // LANES

    strip_e, strip_w, strip_n, strip_s, cond, shares = pl.pallas_call(
        functools.partial(strip_kernel, dims),
        out_shape=[shape(dev_rows, LANES)] * 2
        + [shape(grp_rows, LANES)] * 2
        + [shape(2, cols, rows), shape(nd * share, LANES)],
        in_specs=[SMEM] * 2 + [VMEM] * 3,
        out_specs=[VMEM] * 6,
        scratch_shapes=[vmem(rows // LANES, cols, LANES)],
        compiler_params=PARAMS,
        name="strips",
    )(place, cond_table, load, east_class.T, north_class.T)
    from_n, from_s = exchange(strip_n, strip_s, "grp")
    from_w, from_e = exchange(strip_e, strip_w, "dev")
    tap_count, tap_code, tap_amps = pl.pallas_call(
        functools.partial(tap_kernel, dims, all_cols),
        out_shape=[
            jax.ShapeDtypeStruct((1,), jnp.int32),
            jax.ShapeDtypeStruct((taps.shape[1], LANES), jnp.int32),
            shape(taps.shape[1], LANES),
        ],
        in_specs=[SMEM] + [VMEM] * 2,
        out_specs=[SMEM, VMEM, VMEM],
        compiler_params=SMALL,
        name="taps",
    )(place, taps.T, tap_current.T)
    corner_e_out, corner_w_out = pl.pallas_call(
        functools.partial(corner_kernel, cols),
        out_shape=[shape(corner_rows, LANES)] * 2,
        in_specs=[VMEM] * 2,
        out_specs=[VMEM] * 2,
        compiler_params=SMALL,
        name="corners",
    )(from_n, from_s)
    corner_w, corner_e = exchange(corner_e_out, corner_w_out, "dev")
    gathered = lax.all_to_all(
        shares.reshape(nd, share, LANES), AXES, split_axis=0, concat_axis=0, tiled=True
    )
    factor = coarse_factor(coarse_dims, pc, gathered.reshape(-1, LANES))

    wide0 = cols + 2 * PAD
    ext_rows = rows + 2 * ROW_PAD
    wide1 = cols // 2 + HALO - 2
    rows1 = rows // 2 + ROW_PAD
    lanes0 = lanes_for(ext_rows)
    coef0, coef1 = pl.pallas_call(
        functools.partial(coef_kernel, dims),
        out_shape=[
            shape(3, lanes0 // LANES, wide0, LANES),
            shape(3, lanes_for(lanes0 // 2) // LANES, wide1, LANES),
        ],
        in_specs=[VMEM] * 7,
        out_specs=[VMEM] * 2,
        scratch_shapes=[vmem(wide0, lanes0), vmem(lanes0 // LANES, wide0, LANES)],
        compiler_params=SMALL,
        name="coefs",
    )(cond, from_w, from_e, from_n, from_s, corner_w, corner_e)

    s2_rows = rows1 // 2 * q_cols
    slab_rows = pc * q_rows * q_cols // LANES
    shunts = (SHUNT_CONDUCT, SHUNT_CONDUCT * 4.0)
    s0, p0, s1, p1, slab = pl.pallas_call(
        functools.partial(down_kernel, dims, shunts),
        out_shape=[
            shape(ext_rows * wide0, LANES),
            shape(ext_rows * wide0, LANES),
            shape(rows1 * wide1, LANES),
            shape(rows1 * wide1, LANES),
            shape(nd * slab_rows, LANES),
        ],
        in_specs=[SMEM] * 3 + [HBM] * 3 + [VMEM] * 6,
        out_specs=[HBM] * 2 + [VMEM] * 3,
        scratch_shapes=[
            vmem(ext_rows * wide0, LANES),
            vmem(ext_rows * wide0, LANES),
            vmem(rows, cols, LANES),
            vmem(rows * HALO, LANES),
            vmem(rows * HALO, LANES),
            pltpu.SemaphoreType.DMA((5,)),
            vmem(s2_rows, LANES),
            vmem(GROUP // 2, wide0, LANES),
            vmem(GROUP // 2, wide1, LANES),
        ]
        + rings_for(wide0)
        + rings_for(wide1),
        compiler_params=PARAMS,
        name="fine_down",
    )(tap_count, tap_code.reshape(-1), tap_amps.reshape(-1), load, from_w, from_e, from_n, from_s, corner_w, corner_e, coef0, coef1)

    got = lax.all_to_all(
        slab.reshape(nd, slab_rows, LANES), AXES, split_axis=0, concat_axis=0, tiled=True
    )
    back = coarse_levels(coarse_dims, pc, got.reshape(-1, LANES), factor)
    back = back.reshape(nd, (q_cols + 4) * pc, LANES)
    back = lax.all_to_all(back, AXES, split_axis=0, concat_axis=0, tiled=True)
    pitch2 = -(-(q_cols + 4) // GROUP) * GROUP
    return pl.pallas_call(
        functools.partial(up_kernel, dims, shunts),
        out_shape=shape(rows, cols, LANES),
        in_specs=[VMEM] + [HBM] * 2 + [VMEM] * 4,
        out_specs=VMEM,
        scratch_shapes=[
            vmem(ext_rows * wide0, LANES),
            vmem(ext_rows * wide0, LANES),
            pltpu.SemaphoreType.DMA((2,)),
            vmem((q_rows + 4) * pitch2, LANES),
            vmem(rows1 * wide1, LANES),
            vmem(GROUP, wide1, LANES),
            vmem(GROUP, 2 * wide1, LANES),
        ]
        + rings_for(2 * wide1)
        + rings_for(wide1),
        compiler_params=PARAMS,
        name="fine_up",
    )(back.reshape(-1, LANES), s0, p0, s1, p1, coef0, coef1)


def solution(mesh):
    return jax.shard_map(
        body,
        mesh=mesh,
        in_specs=(P("grp", "dev", None), P("grp", "dev"), P("grp", "dev"), P(), P(), P()),
        out_specs=P("grp", "dev", None),
        check_vma=False,
    )
```

```python
import functools

import jax
import jax.numpy as jnp
from jax import lax
from jax.experimental import pallas as pl
from jax.experimental.pallas import tpu as pltpu
from jax.sharding import PartitionSpec as P


LEVELS = 5
RELAXATION = 0.8
SHUNT_CONDUCT = 0.01
AXES = ("grp", "dev")
HIGH = lax.Precision.HIGHEST

HALO = 10
PAD = 12
ROW_PAD = 16
LANES = 128
GROUP = 8


def exchange(tail, head, axis):
    count = lax.axis_size(axis)
    up = [(i, i + 1) for i in range(count - 1)]
    down = [(i + 1, i) for i in range(count - 1)]
    return lax.ppermute(tail, axis, up), lax.ppermute(head, axis, down)


RING = 4 * GROUP


def wave(
    groups, stop, width, coef, coef_first, spread_weight, shunt, rings, fill, source, middle, finish
):
    ring_e, ring_n, ring_w, ring_a, ring_b, flux_b, again_b, flux_c, turn = rings
    low, high = groups
    per_tile = LANES // GROUP
    for ref in rings:
        ref[...] = jnp.zeros_like(ref)

    def at(ref, row, ahead=0):
        base = pl.multiple_of(lax.rem(row, RING) * width, GROUP)
        return ref[pl.ds(base + ahead, width), :]

    def put(ref, row, value):
        base = pl.multiple_of(lax.rem(row, RING) * width, GROUP)
        ref[pl.ds(base, width), :] = value

    def balance(ring, row, before, slot):
        here = at(ring, row)
        east = at(ring_e, row) * (at(ring, row + 1) - here)
        north = at(ring_n, row) * (at(ring, row, 1) - here)
        turn[slot, pl.ds(GROUP, width), :] = north
        south = turn[slot, pl.ds(GROUP - 1, width), :]
        total = (east - before) + (north - south) + (source(row) - shunt * here)
        return here, east, total

    def go(t, carry):
        g = jnp.minimum(t, high - 1)
        shift = lax.rem(LANES - lax.rem(g, per_tile) * GROUP, LANES)
        kinds = 3 if spread_weight else 2
        found = [
            pltpu.roll(coef[k, g // per_tile, pl.ds(coef_first, width), :], shift, 1)
            for k in range(kinds)
        ]
        east = at(ring_e, g * GROUP + RING - 1)
        for r in range(GROUP):
            row = g * GROUP + r
            west = east
            east, north, *rest = (
                jnp.broadcast_to(x[:, r : r + 1], (width, LANES)) for x in found
            )
            if spread_weight:
                (weight,) = rest
            else:
                south = pltpu.roll(north, 1, 0)
                weight = RELAXATION / ((shunt + east + west) + (north + south))
            put(ring_e, row, east)
            put(ring_n, row, north)
            put(ring_w, row, weight)
            put(ring_a, row, fill(r, row, weight))
        g = jnp.clip(t - 1, low, high - 1)
        flux = jnp.where(t > high, again_b[...], flux_b[...])
        again_b[...] = flux
        for r in range(GROUP):
            row = g * GROUP + r
            here, flux, total = balance(ring_a, row, flux, r)
            value = here + at(ring_w, row) * total
            put(ring_b, row, value)
            middle(row, value)
        flux_b[...] = flux
        g = jnp.clip(t - 2, low, high - 1)
        flux = flux_c[...]
        for r in range(GROUP):
            row = g * GROUP + r
            here, flux, total = balance(ring_b, row, flux, GROUP + r)
            finish(g, r, row, here, total, lambda row=row: at(ring_w, row))
        flux_c[...] = flux
        return carry

    lax.fori_loop(low, stop + 2, go, 0)


def rings_for(width):
    ring = vmem(RING * width + GROUP, LANES)
    return [ring] * 5 + [vmem(width, LANES)] * 3 + [vmem(2 * GROUP, width + GROUP, LANES)]


def strip_kernel(
    dims, place, table, load, east_class, north_class,
    strip_e, strip_w, strip_n, strip_s, cond, shares, held,
):
    rows, cols, nd, _ = dims
    edge = HALO + 1

    def copy(i, carry):
        strip_e[pl.ds(i * HALO, HALO), :] = load[i, cols - HALO :, :]
        strip_w[pl.ds(i * HALO, HALO), :] = load[i, :HALO, :]
        return carry

    lax.fori_loop(0, rows, copy, 0, unroll=8)
    for i in range(HALO):
        strip_n[pl.ds(i * cols, cols), :] = load[rows - HALO + i]
        strip_s[pl.ds(i * cols, cols), :] = load[i]
    coarse = []
    for k, classes in enumerate((east_class, north_class)):
        kind = classes[...]
        value = jnp.zeros(kind.shape, jnp.float32)
        for c in range(table.shape[0]):
            value = jnp.where(kind == c, table[c], value)
        node = lax.broadcasted_iota(jnp.int32, kind.shape, 1 - k)
        turned = jnp.where(node == place[k], 0.0, value)
        cond[k] = turned
        pieces = rows // LANES
        for h in range(pieces):
            at = pl.ds(rows * HALO + k * edge * pieces + h, edge, stride=pieces)
            part = turned[:, h * LANES : (h + 1) * LANES]
            strip_e[at, :] = part[cols - edge :]
            strip_w[at, :] = part[:edge]
        at = pl.ds(cols * HALO + k * cols, cols)
        strip_n[at, :] = pltpu.roll(turned, edge, 1)[:, :LANES]
        strip_s[at, :] = turned[:, :LANES]
        for _ in range(2):
            even, odd = row_pairs(held, turned)
            turned = halve_lanes(even + odd, odd=True) if k == 0 else halve_lanes(odd)
        coarse.append(turned)
    q_rows, q_cols = rows // 4, cols // 4
    per = LANES // q_rows
    group = q_cols // per
    for k, value in enumerate(coarse):
        for jl in range(per):
            shares[pl.ds(k * group, group), pl.ds(jl * q_rows, q_rows)] = value[
                jl * group : (jl + 1) * group, :q_rows
            ]
    mine = shares[pl.ds(0, 2 * group), :]
    for q in range(1, nd):
        shares[pl.ds(q * 2 * group, 2 * group), :] = mine


def corner_kernel(cols, north, south, out_e, out_w):
    edge = HALO + 1
    cond_at = 2 * HALO * HALO
    for ref in (out_e, out_w):
        ref[...] = jnp.zeros_like(ref)
    for end, strip in enumerate((north, south)):
        for i in range(HALO):
            at = pl.ds((end * HALO + i) * HALO, HALO)
            out_e[at, :] = strip[pl.ds((i + 1) * cols - HALO, HALO), :]
            out_w[at, :] = strip[pl.ds(i * cols, HALO), :]
        for k in range(2):
            at = pl.ds(cond_at + (end * 2 + k) * 2 * GROUP, edge)
            first = cols * HALO + k * cols
            out_e[at, :] = strip[pl.ds(first + cols - edge, edge), :]
            out_w[at, :] = strip[pl.ds(first, edge), :]


def coef_kernel(
    dims, cond, west, east, north, south, corner_w, corner_e, coef0, coef1, grid, held
):
    rows, cols, _, _ = dims
    edge = HALO + 1
    wide1 = coef1.shape[2]
    pieces = rows // LANES
    first = ROW_PAD - edge
    grids = []
    for k in range(2):
        grid[...] = jnp.zeros_like(grid)
        grid[pl.ds(PAD, cols), pl.ds(ROW_PAD, rows)] = cond[k]
        for strip, col in ((west, PAD - edge), (east, PAD + cols)):
            for h in range(pieces):
                at = pl.ds(rows * HALO + k * edge * pieces + h, edge, stride=pieces)
                grid[pl.ds(col, edge), pl.ds(ROW_PAD + h * LANES, LANES)] = strip[at, :]
        for end, (strip, row) in enumerate(((north, first), (south, ROW_PAD + rows))):
            at = pl.ds(cols * HALO + k * cols, cols)
            grid[pl.ds(PAD, cols), pl.ds(row, edge)] = strip[at, :][:, :edge]
            at = pl.ds(2 * HALO * HALO + (end * 2 + k) * 2 * GROUP, edge)
            for corner, col in ((corner_w, PAD - edge), (corner_e, PAD + cols)):
                grid[pl.ds(col, edge), pl.ds(row, edge)] = corner[at, :][:, :edge]
        grids.append(grid[...])

    def put(coef, east, west, north, south, shunt):
        weight = RELAXATION / (shunt + east + west + north + south)
        for i, value in enumerate((east, north, weight)):
            for t, piece in enumerate(lane_chunks(value)):
                coef[i, t] = piece

    east, north = grids
    put(coef0, east, pltpu.roll(east, 1, 1), north, pltpu.roll(north, 1, 0), SHUNT_CONDUCT)
    tiles = east.shape[1] // LANES

    def picked(start):
        at = pl.ds(start, wide1, stride=2)
        return jnp.concatenate([held[t, at, :] for t in range(tiles)], axis=1)

    start = PAD - (HALO - 2)
    for t, piece in enumerate(lane_chunks(east)):
        held[t] = piece
    east = halve_lanes(picked(start) + picked(start + 1), odd=True)
    for t, piece in enumerate(lane_chunks(north)):
        held[t] = piece
    north, south = halve_lanes(picked(start + 1)), halve_lanes(picked(start - 1))
    put(coef1, east, pltpu.roll(east, 1, 1), north, south, 4.0 * SHUNT_CONDUCT)


def tap_kernel(dims, all_cols, place, taps, currents, count, codes, amps):
    rows, cols, _, _ = dims
    node, current = taps[...], currents[...]
    lead = node.shape[0]
    row_at = node // all_cols
    i = row_at - place[2]
    j = node - row_at * all_cols - place[3]
    inside = (i >= -HALO) & (i < rows + HALO) & (j >= -HALO) & (j < cols + HALO)
    lane = lax.broadcasted_iota(jnp.int32, node.shape, 1)
    code = ((i + ROW_PAD) * (cols + 2 * PAD) + j + PAD) * LANES + lane
    flags = jnp.where(inside, 1.0, 0.0)
    at, to = iota2(LANES, LANES)
    upto = exact_dot(flags, (at <= to).astype(jnp.float32))
    at, to = iota2(lead, lead)
    before = exact_dot((at > to).astype(jnp.float32), upto)[:, LANES - 1 :]
    slot = jnp.where(inside, (upto + before).astype(jnp.int32) - 1, -1)
    total = jnp.sum(flags).astype(jnp.int32)
    count[0] = total
    codes[...] = jnp.zeros_like(codes)
    amps[...] = jnp.zeros_like(amps)
    wanted = lax.broadcasted_iota(jnp.int32, (LANES, LANES), 0)
    code = code.astype(jnp.float32)

    def fill(chunk, carry):
        found = jnp.zeros((LANES, LANES), jnp.float32)
        amount = jnp.zeros((LANES, LANES), jnp.float32)
        for k in range(lead):
            hit = wanted + chunk * LANES == jnp.broadcast_to(slot[k : k + 1], wanted.shape)
            found += jnp.where(hit, jnp.broadcast_to(code[k : k + 1], wanted.shape), 0.0)
            amount += jnp.where(hit, jnp.broadcast_to(current[k : k + 1], wanted.shape), 0.0)
        codes[pl.ds(chunk, 1), :] = jnp.sum(found.T, axis=0, keepdims=True).astype(jnp.int32)
        amps[pl.ds(chunk, 1), :] = jnp.sum(amount.T, axis=0, keepdims=True)
        return carry

    lax.fori_loop(0, (total + LANES - 1) // LANES, fill, 0)


def down_kernel(
    dims, shunts, tap_count, tap_code, tap_amps, own_hbm, west_hbm, east_hbm, north, south,
    corner_w, corner_e, coef0, coef1, s0_out, p0_out, s1, p1, slab, s0, p0, own, west, east, sems,
    s2, pair, pair1, *rings,
):
    rows, cols, nd, pc = dims
    wide = cols + 2 * PAD
    rings0, rings1 = rings[:9], rings[9:]

    moves = [
        pltpu.make_async_copy(source.at[pl.ds(0, here.shape[0])], here, sems.at[k])
        for k, (source, here) in enumerate(((own_hbm, own), (west_hbm, west), (east_hbm, east)))
    ]
    for move in moves:
        move.start()
    s0[...] = jnp.zeros_like(s0)
    for move in moves:
        move.wait()
    first = ROW_PAD - HALO

    def copy_own(i, carry):
        base = (i + ROW_PAD) * wide
        s0[pl.ds(base + PAD, cols), :] = -own[i]
        s0[pl.ds(base + PAD - HALO, HALO), :] = -west[pl.ds(i * HALO, HALO), :]
        s0[pl.ds(base + PAD + cols, HALO), :] = -east[pl.ds(i * HALO, HALO), :]
        return carry

    lax.fori_loop(0, rows, copy_own, 0, unroll=8)
    for k, (strip, base) in enumerate(((north, first), (south, ROW_PAD + rows))):
        for i in range(HALO):
            at = (base + i) * wide + PAD
            corner = pl.ds((k * HALO + i) * HALO, HALO)
            s0[pl.ds(at, cols), :] = -strip[i * cols : (i + 1) * cols, :]
            s0[pl.ds(at - HALO, HALO), :] = -corner_w[corner, :]
            s0[pl.ds(at + cols, HALO), :] = -corner_e[corner, :]

    lane = lax.broadcasted_iota(jnp.int32, (GROUP, LANES), 1)
    sub = lax.broadcasted_iota(jnp.int32, (GROUP, LANES), 0)

    def add_tap(k, carry):
        code = tap_code[k]
        node = code // LANES
        base = pl.multiple_of(node // GROUP * GROUP, GROUP)
        hit = (lane == lax.rem(code, LANES)) & (sub == node - base)
        s0[pl.ds(base, GROUP), :] += jnp.where(hit, tap_amps[k], 0.0)
        return carry

    lax.fori_loop(0, tap_count[0], add_tap, 0)
    save_s0 = pltpu.make_async_copy(s0, s0_out, sems.at[3])
    save_p0 = pltpu.make_async_copy(p0, p0_out, sems.at[4])
    save_s0.start()

    def smooth_and_restrict(source, pre, coef, spread_weight, shunt, pair, rings, store):
        width = pair.shape[1]
        held = []

        def row_of(ref, row):
            return ref[pl.ds(pl.multiple_of(row * width, GROUP), width), :]

        def middle(row, value):
            pre[pl.ds(pl.multiple_of(row * width, GROUP), width), :] = value

        def finish(g, r, row, here, total, weight):
            if r % 2 == 0:
                held.append(total)
            else:
                pair[r // 2] = held.pop() + total
                store(g * (GROUP // 2) + r // 2, r // 2)

        groups = source.shape[0] // width // GROUP
        wave(
            (0, groups), groups - 1, width, coef, 0, spread_weight, shunt, rings,
            lambda r, row, weight: weight * row_of(source, row),
            lambda row: row_of(source, row), middle, finish,
        )

    half = pair1.shape[1]
    start = PAD - (HALO - 2)

    def store1(k, m):
        s1[pl.ds(pl.multiple_of(k * half, GROUP), half), :] = (
            pair[m, pl.ds(start, half, stride=2), :] + pair[m, pl.ds(start + 1, half, stride=2), :]
        )

    smooth_and_restrict(s0, p0, coef0, False, shunts[0], pair, rings0, store1)
    save_p0.start()
    quarter = cols // 4

    def store2(k, m):
        s2[pl.ds(pl.multiple_of(k * quarter, quarter), quarter), :] = (
            pair1[m, pl.ds(4, quarter, stride=2), :] + pair1[m, pl.ds(5, quarter, stride=2), :]
        )

    smooth_and_restrict(s1, p1, coef1, True, shunts[1], pair1, rings1, store2)
    rows2 = rows // 4
    per = LANES // rows2
    groups = quarter // per
    for jp in range(groups):
        parts = [
            s2[pl.ds(ROW_PAD // 4 * quarter + jl * groups + jp, rows2, stride=quarter), :]
            for jl in range(per)
        ]
        turned = jnp.concatenate(parts, axis=0).T
        for p in range(pc):
            slab[pl.ds(jp * pc + p, nd, stride=groups * pc), :] = turned[p * nd : (p + 1) * nd]
    save_s0.wait()
    save_p0.wait()


def up_kernel(
    dims, shunts, back, s0_hbm, p0_hbm, s1, p1, coef0, coef1, out, s0, p0, sems, x2, c1, twice1,
    twice0, *rings,
):
    rows, cols, nd, pc = dims
    wide = cols + 2 * PAD
    quarter = cols // 4
    wide2 = quarter + 4
    width1 = 2 * wide2
    width0 = 2 * width1
    rows2 = rows // 4 + 4
    pitch2 = x2.shape[0] // rows2
    rings0, rings1 = rings[:9], rings[9:]
    moves = [
        pltpu.make_async_copy(far, near, sems.at[k])
        for k, (far, near) in enumerate(((s0_hbm, s0), (p0_hbm, p0)))
    ]
    for move in moves:
        move.start()
    for jw in range(wide2):
        parts = [back[pl.ds(jw * pc + p, nd, stride=wide2 * pc), :] for p in range(pc)]
        turned = jnp.concatenate(parts, axis=0).T
        x2[pl.ds(jw, rows2, stride=pitch2), :] = turned[:rows2]

    def lifted(twice, slot, x):
        count = x.shape[0]
        twice[slot, pl.ds(0, count, stride=2), :] = x
        twice[slot, pl.ds(1, count, stride=2), :] = x
        return twice[slot]

    def fill1(r, row, weight):
        k = jnp.clip(row // 2 - 2, 0, rows2 - 1)
        x = x2[pl.ds(pl.multiple_of(k * pitch2, GROUP), pitch2), :][:wide2]
        return p1[pl.ds(pl.multiple_of(row * width1, GROUP), width1), :] + lifted(
            twice1, r, x
        )

    def source1(row):
        return s1[pl.ds(pl.multiple_of(row * width1, GROUP), width1), :]

    def finish1(g, r, row, here, total, weight):
        c1[pl.ds(pl.multiple_of(row * width1, GROUP), width1), :] = here + weight() * total

    groups1 = s1.shape[0] // width1 // GROUP
    wave(
        (0, groups1), groups1, width1, coef1, 0, True, shunts[1], rings1,
        fill1, source1, lambda row, value: None, finish1,
    )

    start = PAD - (HALO - 2)

    def fill0(r, row, weight):
        x = c1[pl.ds(pl.multiple_of(row // 2 * width1, GROUP), width1), :]
        return p0[pl.ds(row * wide + start, width0), :] + lifted(twice0, r, x)

    def source0(row):
        return s0[pl.ds(row * wide + start, width0), :]

    first, last = ROW_PAD // GROUP, (ROW_PAD + rows) // GROUP
    for move in moves:
        move.wait()

    def finish0(g, r, row, here, total, weight):
        done = here + weight() * total
        row = jnp.clip(row - ROW_PAD, r, rows - GROUP + r)
        out[row] = done[HALO - 2 : HALO - 2 + cols]

    wave(
        (first - 1, last + 1), last, width0, coef0, start, False, shunts[0], rings0,
        fill0, source0, lambda row, value: None, finish0,
    )


VMEM = pl.BlockSpec(memory_space=pltpu.VMEM)
SMEM = pl.BlockSpec(memory_space=pltpu.SMEM)
HBM = pl.BlockSpec(memory_space=pltpu.HBM)
PARAMS = pltpu.CompilerParams(vmem_limit_bytes=60 * 1024 * 2**10)


SMALL = pltpu.CompilerParams(vmem_limit_bytes=16 * 2**20)


def shape(*dims):
    return jax.ShapeDtypeStruct(dims, jnp.float32)


def vmem(*dims):
    return pltpu.VMEM(dims, jnp.float32)


def lane_chunks(x):
    return [x[:, i : i + LANES] for i in range(0, x.shape[1], LANES)]


def block_column(x, k):
    size = x.shape[0]
    lane = lax.broadcasted_iota(jnp.int32, (size, LANES), 1)
    at = lane // size * size + k
    take = functools.partial(jnp.take_along_axis, axis=1, mode="promise_in_bounds")
    return jnp.concatenate([take(c, at) for c in lane_chunks(x)], axis=1)


def block_rows(held, x):
    held[...] = x

    def row(k):
        return jnp.broadcast_to(held[pl.ds(k, 1), :], x.shape)

    return row


def over(size, step, start):
    return lax.fori_loop(0, size, step, start, unroll=size <= GROUP)


def block_product(held, x, *others):
    rows = [block_rows(h, y) for h, y in zip(held, others)]

    def step(k, totals):
        column = block_column(x, k)
        return tuple(t + column * row(k) for t, row in zip(totals, rows))

    return over(x.shape[0], step, tuple(jnp.zeros_like(x) for _ in others))


def block_inverse(held, x):
    size, _ = x.shape
    inner = lax.broadcasted_iota(jnp.int32, x.shape, 1) % size
    row_id = lax.broadcasted_iota(jnp.int32, x.shape, 0)

    def step(k, x):
        row = block_rows(held[0], x)(k)
        column = block_column(x, k)
        pivot = block_rows(held[1], column)(k)
        scaled = jnp.where(inner == k, 1.0, row) / pivot
        rest = jnp.where(inner == k, 0.0, x) - column * scaled
        return jnp.where(row_id == k, scaled, rest)

    return over(size, step, x)


def ahead(x, blocks):
    lanes = x.shape[1]
    return pltpu.roll(x, (-blocks * x.shape[0]) % lanes, 1)


def exact_dot(x, y):
    return jnp.dot(x, y, precision=HIGH, preferred_element_type=jnp.float32)


def iota2(rows, cols):
    return (
        lax.broadcasted_iota(jnp.int32, (rows, cols), 0),
        lax.broadcasted_iota(jnp.int32, (rows, cols), 1),
    )


def lanes_for(count):
    return -(-count // LANES) * LANES


def halve_lanes(x, odd=False):
    count = x.shape[1]
    fine, coarse = iota2(count, lanes_for(count // 2))
    hit = fine == 2 * coarse + 1 if odd else fine // 2 == coarse
    return exact_dot(x, hit.astype(jnp.float32))


def double_lanes(x, count):
    coarse, fine = iota2(x.shape[1], count)
    return exact_dot(x, (fine // 2 == coarse).astype(jnp.float32))


def row_pairs(held, x):
    rows = x.shape[0]
    for t, piece in enumerate(lane_chunks(x)):
        held[t, pl.ds(0, rows), :] = piece
    return [
        jnp.concatenate(
            [held[t, pl.ds(k, rows // 2, stride=2), :] for t in range(x.shape[1] // LANES)], axis=1
        )
        for k in range(2)
    ]


def double_rows(held, x):
    rows = x.shape[0]
    for t, piece in enumerate(lane_chunks(x)):
        for k in range(2):
            held[t, pl.ds(k, rows, stride=2), :] = piece
    return jnp.concatenate(
        [held[t, pl.ds(0, 2 * rows), :] for t in range(x.shape[1] // LANES)], axis=1
    )


def place_blocks(dims, from_ref, pitch, to_ref, sets):
    ng, nd_axis, q_rows, q_cols = dims
    per = LANES // q_rows
    group = q_cols // per
    for g in range(ng):
        for d in range(nd_axis):
            for first, stride, base in sets:
                at = (g * nd_axis + d) * pitch + first
                piece = from_ref[pl.ds(at, group, stride=stride), :]
                for jl in range(per):
                    to_ref[
                        pl.ds(base + d * q_cols + jl * group, group), pl.ds(g * q_rows, q_rows)
                    ] = piece[:, jl * q_rows : (jl + 1) * q_rows]


def factor_kernel(dims, pc, gathered, *refs):
    levels = LEVELS - 2
    coefs, (parts, last), (grid, spare, *held) = refs[:levels], refs[levels:levels + 2], refs[levels + 2:]
    ng, nd_axis, q_rows, q_cols = dims
    nj, ni = nd_axis * q_cols, ng * q_rows
    group = q_cols * q_rows // LANES
    place_blocks(dims, gathered, 2 * group, grid, [(0, 1, 0), (group, 1, nj)])
    east, north = grid[pl.ds(0, nj), :], grid[pl.ds(nj, nj), :]
    for k in range(LEVELS - 1):
        shunt = SHUNT_CONDUCT * 4.0 ** (k + 2)
        west, south = pltpu.roll(east, 1, 1), pltpu.roll(north, 1, 0)
        diag = shunt + east + west + north + south
        if k == levels:
            break
        for i, part in enumerate((east, north, RELAXATION / diag)):
            for p in range(pc):
                coefs[k][i, pl.ds(p * nj, nj), :] = part
        even, odd = row_pairs(spare, east)
        east = halve_lanes(even + odd, odd=True)
        even, odd = row_pairs(spare, north)
        north = halve_lanes(odd)
        nj, ni = nj // 2, ni // 2
    size, count = nj, ni * nj
    at, lane = iota2(east.shape[1], count)
    repeat = (lane // size == at).astype(jnp.float32)
    row, col = iota2(size, count)
    col = col % size
    d = jnp.where(col == row, exact_dot(diag, repeat), 0.0)
    d = d - jnp.where(col == row + 1, exact_dot(north, repeat), 0.0)
    d = d - jnp.where(col == row - 1, exact_dot(south, repeat), 0.0)
    c = jnp.where(col == row, -exact_dot(east, repeat), 0.0)
    ct = c
    stride = 1
    level = 0
    while stride * size < count:
        inverse = block_inverse(held, d)
        (r,) = block_product(held, c, ahead(inverse, stride))
        (lx,) = block_product(held, ct, inverse)
        left, lead = ahead(lx, -stride), ahead(lx, stride)
        for i, part in enumerate((r, left, inverse, c, ahead(ct, -stride))):
            parts[level, i] = part
        first, new_c = block_product(held, r, ct, ahead(c, stride))
        (second,) = block_product(held, left, ahead(c, -stride))
        (new_ct,) = block_product(held, lead, ct)
        d = d - first - second
        c, ct = -new_c, -new_ct
        stride *= 2
        level += 1
    last[...] = block_inverse(held, d)


def reduce_and_solve(held, f, parts, last):
    size = f.shape[0]
    block = lax.broadcasted_iota(jnp.int32, f.shape, 1) // size
    levels = parts.shape[0]
    for level in range(levels):
        s = 2**level
        (a,) = block_product(held, parts[level, 0], ahead(f, s))
        (b,) = block_product(held, parts[level, 1], ahead(f, -s))
        f = jnp.where(block % (2 * s) == 0, f - a - b, f)
    (x,) = block_product(held, last[...], f)
    for level in reversed(range(levels)):
        s = 2**level
        (a,) = block_product(held, parts[level, 3], ahead(x, s))
        (b,) = block_product(held, parts[level, 4], ahead(x, -s))
        (new,) = block_product(held, parts[level, 2], f - a - b)
        x = jnp.where(block % (2 * s) == s, new, x)
    return x


def grid_residual(v, source, coef, shunt):
    lanes, rows = v.shape[1], v.shape[0]
    east = coef[0] * (pltpu.roll(v, lanes - 1, 1) - v)
    north = coef[1] * (pltpu.roll(v, rows - 1, 0) - v)
    total = (east - pltpu.roll(east, 1, 1)) + (north - pltpu.roll(north, 1, 0))
    return total + (source - shunt * v)


def coarse_kernel(dims, pc, got, *refs):
    levels = LEVELS - 2
    coefs, (parts, last, back) = refs[:levels], refs[levels : levels + 3]
    grid, spare, shifted, shifted_odd, *held = refs[levels + 3 :]
    ng, nd_axis, q_rows, q_cols = dims
    nj, ni = nd_axis * q_cols, ng * q_rows
    pitch = got.shape[0] // (ng * nd_axis)
    place_blocks(dims, got, pitch, grid, [(p, pc, p * nj) for p in range(pc)])
    source = grid[...]
    stored = []
    for k in range(levels):
        shunt = SHUNT_CONDUCT * 4.0 ** (k + 2)
        coef = coefs[k]
        start = coef[2] * source
        pre = start + coef[2] * grid_residual(start, source, coef, shunt)
        rest = grid_residual(pre, source, coef, shunt)
        stored.append((pre, source, shunt, coef))
        even, odd = row_pairs(spare, rest)
        source = halve_lanes(even + odd)
    size = source.shape[0] // pc
    blocks = ni // 2**levels
    at, lane = iota2(source.shape[1], size * blocks)
    f = None
    picks = [(lane == at * size + p).astype(jnp.float32) for p in range(pc)]
    for p, pick in enumerate(picks):
        part = exact_dot(source[p * size : (p + 1) * size], pick)
        f = part if f is None else f + part
    x = reduce_and_solve(held, f, parts, last)
    fix = jnp.concatenate([exact_dot(x, pick.T) for pick in picks], axis=0)
    for pre, source, shunt, coef in reversed(stored):
        lanes = pre.shape[1]
        v = pre + double_rows(spare, double_lanes(fix, lanes))
        for _ in range(2):
            v = v + coef[2] * grid_residual(v, source, coef, shunt)
        fix = v
    shifted[...] = jnp.zeros_like(shifted)
    rows_p = shifted.shape[0] // pc
    wide = jnp.concatenate([fix, jnp.zeros((fix.shape[0], LANES), jnp.float32)], axis=1)
    wide = pltpu.roll(wide, 2, 1)
    for p in range(pc):
        shifted[pl.ds(p * rows_p + 2, nj), :] = wide[p * nj : (p + 1) * nj]
    lanes = shifted.shape[1]
    shifted_odd[...] = pltpu.roll(shifted[...], lanes - LANES // 2, 1)
    window = q_cols + 4
    for g in range(ng):
        lane_at = g * q_rows
        ref = shifted if lane_at % LANES == 0 else shifted_odd
        lane_at = lane_at // LANES * LANES
        for d in range(nd_axis):
            for p in range(pc):
                piece = ref[pl.ds(p * rows_p + d * q_cols, window), pl.ds(lane_at, LANES)]
                at = (g * nd_axis + d) * window * pc + p
                back[pl.ds(at, window, stride=pc), :] = piece


def coarse_factor(dims, pc, gathered):
    ng, nd_axis, q_rows, q_cols = dims
    nj, ni = nd_axis * q_cols, ng * q_rows
    coefs = []
    for k in range(LEVELS - 2):
        coefs.append(shape(3, pc * nj >> k, lanes_for(ni >> k)))
    size, blocks = nj >> (LEVELS - 2), ni >> (LEVELS - 2)
    flat = (size, blocks * size)
    out = pl.pallas_call(
        functools.partial(factor_kernel, dims, pc),
        out_shape=coefs + [shape(blocks.bit_length() - 1, 5, *flat), shape(*flat)],
        in_specs=[VMEM],
        out_specs=[VMEM] * (len(coefs) + 2),
        scratch_shapes=[vmem(2 * nj, ni), vmem(ni // LANES, nj, LANES)] + [vmem(*flat)] * 2,
        compiler_params=SMALL,
        name="coarse_factor",
    )(gathered)
    return out


def coarse_levels(dims, pc, got, factor):
    ng, nd_axis, q_rows, q_cols = dims
    nj, ni = nd_axis * q_cols, ng * q_rows
    flat = factor[-1].shape
    padded = (pc * (nj + GROUP), ni + LANES)
    return pl.pallas_call(
        functools.partial(coarse_kernel, dims, pc),
        out_shape=shape(ng * nd_axis * (q_cols + 4) * pc, LANES),
        in_specs=[VMEM] * (len(factor) + 1),
        out_specs=VMEM,
        scratch_shapes=[
            vmem(pc * nj, ni), vmem(ni // LANES, pc * nj, LANES), vmem(*padded), vmem(*padded)
        ]
        + [vmem(*flat)] * 2,
        compiler_params=SMALL,
        name="coarse_levels",
    )(got, *factor)


def body(load, east_class, north_class, cond_table, taps, tap_current):
    rows, cols, cands = load.shape
    ng, nd_axis = lax.axis_size("grp"), lax.axis_size("dev")
    nd = ng * nd_axis
    pc = cands // nd
    row_start = lax.axis_index("grp") * rows
    col_start = lax.axis_index("dev") * cols
    all_rows, all_cols = ng * rows, nd_axis * cols
    edge = HALO + 1
    dims = (rows, cols, nd, pc)

    q_rows, q_cols = rows // 4, cols // 4
    coarse_dims = (ng, nd_axis, q_rows, q_cols)
    place = jnp.stack(
        [all_rows - 1 - row_start, all_cols - 1 - col_start, row_start, col_start]
    ).astype(jnp.int32)
    dev_rows = rows * HALO + 2 * edge * rows // LANES
    grp_rows = cols * HALO + 2 * cols
    corner_rows = 2 * HALO * HALO + 8 * GROUP
    share = 2 * q_rows * q_cols // LANES

    strip_e, strip_w, strip_n, strip_s, cond, shares = pl.pallas_call(
        functools.partial(strip_kernel, dims),
        out_shape=[shape(dev_rows, LANES)] * 2
        + [shape(grp_rows, LANES)] * 2
        + [shape(2, cols, rows), shape(nd * share, LANES)],
        in_specs=[SMEM] * 2 + [VMEM] * 3,
        out_specs=[VMEM] * 6,
        scratch_shapes=[vmem(rows // LANES, cols, LANES)],
        compiler_params=PARAMS,
        name="strips",
    )(place, cond_table, load, east_class.T, north_class.T)
    from_n, from_s = exchange(strip_n, strip_s, "grp")
    from_w, from_e = exchange(strip_e, strip_w, "dev")
    tap_count, tap_code, tap_amps = pl.pallas_call(
        functools.partial(tap_kernel, dims, all_cols),
        out_shape=[
            jax.ShapeDtypeStruct((1,), jnp.int32),
            jax.ShapeDtypeStruct((taps.shape[1], LANES), jnp.int32),
            shape(taps.shape[1], LANES),
        ],
        in_specs=[SMEM] + [VMEM] * 2,
        out_specs=[SMEM, VMEM, VMEM],
        compiler_params=SMALL,
        name="taps",
    )(place, taps.T, tap_current.T)
    corner_e_out, corner_w_out = pl.pallas_call(
        functools.partial(corner_kernel, cols),
        out_shape=[shape(corner_rows, LANES)] * 2,
        in_specs=[VMEM] * 2,
        out_specs=[VMEM] * 2,
        compiler_params=SMALL,
        name="corners",
    )(from_n, from_s)
    corner_w, corner_e = exchange(corner_e_out, corner_w_out, "dev")
    gathered = lax.all_to_all(
        shares.reshape(nd, share, LANES), AXES, split_axis=0, concat_axis=0, tiled=True
    )
    factor = coarse_factor(coarse_dims, pc, gathered.reshape(-1, LANES))

    wide0 = cols + 2 * PAD
    ext_rows = rows + 2 * ROW_PAD
    wide1 = cols // 2 + HALO - 2
    rows1 = rows // 2 + ROW_PAD
    lanes0 = lanes_for(ext_rows)
    coef0, coef1 = pl.pallas_call(
        functools.partial(coef_kernel, dims),
        out_shape=[
            shape(3, lanes0 // LANES, wide0, LANES),
            shape(3, lanes_for(lanes0 // 2) // LANES, wide1, LANES),
        ],
        in_specs=[VMEM] * 7,
        out_specs=[VMEM] * 2,
        scratch_shapes=[vmem(wide0, lanes0), vmem(lanes0 // LANES, wide0, LANES)],
        compiler_params=SMALL,
        name="coefs",
    )(cond, from_w, from_e, from_n, from_s, corner_w, corner_e)

    s2_rows = rows1 // 2 * q_cols
    slab_rows = pc * q_rows * q_cols // LANES
    shunts = (SHUNT_CONDUCT, SHUNT_CONDUCT * 4.0)
    s0, p0, s1, p1, slab = pl.pallas_call(
        functools.partial(down_kernel, dims, shunts),
        out_shape=[
            shape(ext_rows * wide0, LANES),
            shape(ext_rows * wide0, LANES),
            shape(rows1 * wide1, LANES),
            shape(rows1 * wide1, LANES),
            shape(nd * slab_rows, LANES),
        ],
        in_specs=[SMEM] * 3 + [HBM] * 3 + [VMEM] * 6,
        out_specs=[HBM] * 2 + [VMEM] * 3,
        scratch_shapes=[
            vmem(ext_rows * wide0, LANES),
            vmem(ext_rows * wide0, LANES),
            vmem(rows, cols, LANES),
            vmem(rows * HALO, LANES),
            vmem(rows * HALO, LANES),
            pltpu.SemaphoreType.DMA((5,)),
            vmem(s2_rows, LANES),
            vmem(GROUP // 2, wide0, LANES),
            vmem(GROUP // 2, wide1, LANES),
        ]
        + rings_for(wide0)
        + rings_for(wide1),
        compiler_params=PARAMS,
        name="fine_down",
    )(tap_count, tap_code.reshape(-1), tap_amps.reshape(-1), load, from_w, from_e, from_n, from_s, corner_w, corner_e, coef0, coef1)

    got = lax.all_to_all(
        slab.reshape(nd, slab_rows, LANES), AXES, split_axis=0, concat_axis=0, tiled=True
    )
    back = coarse_levels(coarse_dims, pc, got.reshape(-1, LANES), factor)
    back = back.reshape(nd, (q_cols + 4) * pc, LANES)
    back = lax.all_to_all(back, AXES, split_axis=0, concat_axis=0, tiled=True)
    pitch2 = -(-(q_cols + 4) // GROUP) * GROUP
    return pl.pallas_call(
        functools.partial(up_kernel, dims, shunts),
        out_shape=shape(rows, cols, LANES),
        in_specs=[VMEM] + [HBM] * 2 + [VMEM] * 4,
        out_specs=VMEM,
        scratch_shapes=[
            vmem(ext_rows * wide0, LANES),
            vmem(ext_rows * wide0, LANES),
            pltpu.SemaphoreType.DMA((2,)),
            vmem((q_rows + 4) * pitch2, LANES),
            vmem(rows1 * wide1, LANES),
            vmem(GROUP, wide1, LANES),
            vmem(GROUP, 2 * wide1, LANES),
        ]
        + rings_for(2 * wide1)
        + rings_for(wide1),
        compiler_params=PARAMS,
        name="fine_up",
    )(back.reshape(-1, LANES), s0, p0, s1, p1, coef0, coef1)


def solution(mesh):
    return jax.shard_map(
        body,
        mesh=mesh,
        in_specs=(P("grp", "dev", None), P("grp", "dev"), P("grp", "dev"), P(), P(), P()),
        out_specs=P("grp", "dev", None),
        check_vma=False,
    )
```
